8 devices in a mesh: dp: 1 (over z), tp: 2 (over y), cp: 4 (over x, core).
Axes of the slice: x: 2, y: 2, z: 1, core: 2. Of those that a mesh axis runs over, the one named last changes fastest.
Arguments:
- tokens: bfloat16 [1024, 2048], P(('dp', 'tp', 'cp'))
- norm_attn: bfloat16 [2, 2048], replicated
- norm_mlp: bfloat16 [2, 2048], replicated
- w_q: bfloat16 [2, 2048, 32, 64], P(None, None, 'tp')
- w_k: bfloat16 [2, 2048, 512], P(None, None, 'tp')
- w_v: bfloat16 [2, 2048, 512], P(None, None, 'tp')
- w_o: bfloat16 [2, 32, 64, 2048], P(None, 'tp')
- w_gate: bfloat16 [2, 2048, 8192], P(None, None, 'tp')
- w_up: bfloat16 [2, 2048, 8192], P(None, None, 'tp')
- w_down: bfloat16 [2, 8192, 2048], P(None, 'tp')
Outputs:
- output: bfloat16 [1024, 2048], P(('dp', 'tp', 'cp'))
All inputs are finite; a program needn't handle non-finite values.
Results may differ from the reference program's by a relative error of at most 0.02.
Values are sent between devices in bfloat16 or wider.
A program may use at most 1 GiB of HBM per device.

```python
import math
import jax
import jax.numpy as jnp
from jax import lax

D = 2048
FF = 8192
HEADS = 32
KV_HEADS = 8
HEAD = 64
SEQ = 1024
SEGMENT = 64
LAYERS = 2

GROUP = HEADS // KV_HEADS
GROUP_DEVICES = SEQ // (2 * SEGMENT)


def row_positions():
    row_idx = jnp.arange(SEQ)
    device_idx = row_idx // (2 * SEGMENT)
    offset = row_idx % (2 * SEGMENT)
    seg_idx = jnp.where(offset < SEGMENT, device_idx, 2 * GROUP_DEVICES - 1 - device_idx)
    return seg_idx * SEGMENT + offset % SEGMENT


def rms_norm(hidden, gain):
    hidden_f = hidden.astype(jnp.float32)
    inv_rms = lax.rsqrt(jnp.mean(hidden_f * hidden_f, axis=-1, keepdims=True) + 1e-5)
    return (hidden_f * inv_rms * gain.astype(jnp.float32)).astype(jnp.bfloat16)


def rotary(values, positions):
    half_dim = values.shape[-1] // 2
    inv_freq = 500000.0 ** (-(jnp.arange(half_dim, dtype=jnp.float32) * 2.0 / values.shape[-1]))
    angles = positions.astype(jnp.float32)[:, None] * inv_freq[None, :]
    cos_ang = jnp.cos(angles)[:, None, :]
    sin_ang = jnp.sin(angles)[:, None, :]
    first = values[..., :half_dim]
    second = values[..., half_dim:]
    return jnp.concatenate([first * cos_ang - second * sin_ang, second * cos_ang + first * sin_ang], axis=-1)


def attention(queries, keys, value_rows, positions):
    keys_f = keys.astype(jnp.float32)
    values_f = value_rows.astype(jnp.float32)
    q_blocks = queries.reshape(SEQ // SEGMENT, SEGMENT, KV_HEADS, GROUP, HEAD)
    pos_blocks = positions.reshape(SEQ // SEGMENT, SEGMENT)
    scale = 1.0 / math.sqrt(HEAD)

    def one_block(block):
        q_blk, pos_blk = block
        scores = jnp.einsum('bkgd,tkd->bkgt', q_blk.astype(jnp.float32), keys_f) * scale
        visible = positions[None, None, None, :] <= pos_blk[:, None, None, None]
        scores = jnp.where(visible, scores, -jnp.inf)
        row_max = jnp.max(scores, axis=-1, keepdims=True)
        weights = jnp.exp(scores - row_max)
        row_sum = jnp.sum(weights, axis=-1, keepdims=True)
        mixed = jnp.einsum('bkgt,tkd->bkgd', weights.astype(jnp.bfloat16).astype(jnp.float32), values_f)
        return (mixed / row_sum).astype(jnp.bfloat16)

    return lax.map(one_block, (q_blocks, pos_blocks)).reshape(SEQ, HEADS * HEAD)


def layer(hidden, params, positions):
    norm_attn, norm_mlp, w_q, w_k, w_v, w_o, w_gate, w_up, w_down = params
    normed = rms_norm(hidden, norm_attn)
    q_proj = jnp.dot(normed, w_q.reshape(D, HEADS * HEAD), preferred_element_type=jnp.float32)
    queries = rotary(q_proj.reshape(SEQ, HEADS, HEAD), positions).astype(jnp.bfloat16)
    k_proj = jnp.dot(normed, w_k, preferred_element_type=jnp.float32)
    keys = rotary(k_proj.reshape(SEQ, KV_HEADS, HEAD), positions).astype(jnp.bfloat16)
    value_rows = jnp.dot(normed, w_v, preferred_element_type=jnp.float32).astype(jnp.bfloat16).reshape(SEQ, KV_HEADS, HEAD)
    mixed = attention(queries.reshape(SEQ, KV_HEADS, GROUP, HEAD), keys, value_rows, positions)
    attn_out = jnp.dot(mixed, w_o.reshape(HEADS * HEAD, D), preferred_element_type=jnp.float32)
    hidden_mid = (hidden.astype(jnp.float32) + attn_out).astype(jnp.bfloat16)
    normed_mlp = rms_norm(hidden_mid, norm_mlp)
    gate_pre = jnp.dot(normed_mlp, w_gate, preferred_element_type=jnp.float32)
    up_proj = jnp.dot(normed_mlp, w_up, preferred_element_type=jnp.float32)
    hidden_act = (jax.nn.silu(gate_pre) * up_proj).astype(jnp.bfloat16)
    mlp_out = jnp.dot(hidden_act, w_down, preferred_element_type=jnp.float32)
    return (hidden_mid.astype(jnp.float32) + mlp_out).astype(jnp.bfloat16)


def setup_inputs(seed: int = 0, part: int = 0) -> dict:
    key_list = jax.random.split(jax.random.key(seed), 10)
    score_gain = math.sqrt(max(math.log(SEQ) - 2.0, 1.0))
    tokens = jax.random.normal(jax.random.fold_in(key_list[0], part), (SEQ, D), jnp.float32)
    norm_attn = 1.0 + 0.3 * jax.random.normal(key_list[1], (LAYERS, D), jnp.float32)
    norm_mlp = 1.0 + 0.3 * jax.random.normal(key_list[2], (LAYERS, D), jnp.float32)
    w_q = jax.random.normal(key_list[3], (LAYERS, D, HEADS, HEAD), jnp.float32) * (score_gain / math.sqrt(D))
    w_k = jax.random.normal(key_list[4], (LAYERS, D, KV_HEADS * HEAD), jnp.float32) / math.sqrt(D)
    w_v = jax.random.normal(key_list[5], (LAYERS, D, KV_HEADS * HEAD), jnp.float32) / math.sqrt(D)
    w_o = jax.random.normal(key_list[6], (LAYERS, HEADS, HEAD, D), jnp.float32) / math.sqrt(HEADS * HEAD)
    w_gate = jax.random.normal(key_list[7], (LAYERS, D, FF), jnp.float32) / math.sqrt(D)
    w_up = jax.random.normal(key_list[8], (LAYERS, D, FF), jnp.float32) / math.sqrt(D)
    w_down = jax.random.normal(key_list[9], (LAYERS, FF, D), jnp.float32) * (1.5 / math.sqrt(FF))
    return dict(
        tokens=tokens.astype(jnp.bfloat16),
        norm_attn=norm_attn.astype(jnp.bfloat16),
        norm_mlp=norm_mlp.astype(jnp.bfloat16),
        w_q=w_q.astype(jnp.bfloat16),
        w_k=w_k.astype(jnp.bfloat16),
        w_v=w_v.astype(jnp.bfloat16),
        w_o=w_o.astype(jnp.bfloat16),
        w_gate=w_gate.astype(jnp.bfloat16),
        w_up=w_up.astype(jnp.bfloat16),
        w_down=w_down.astype(jnp.bfloat16),
    )


def reference(tokens, norm_attn, norm_mlp, w_q, w_k, w_v, w_o, w_gate, w_up, w_down):
    positions = row_positions()

    def layer_step(hidden, params):
        return layer(hidden, params, positions), None

    stacked = (norm_attn, norm_mlp, w_q, w_k, w_v, w_o, w_gate, w_up, w_down)
    return lax.scan(layer_step, tokens, stacked)[0]
```

```python
import math
import jax
import jax.numpy as jnp
from jax import lax
from jax.sharding import PartitionSpec as P, NamedSharding


def rms_norm(hidden, gain):
    hidden_f = hidden.astype(jnp.float32)
    inv_rms = lax.rsqrt(jnp.mean(hidden_f * hidden_f, axis=-1, keepdims=True) + 1e-5)
    return (hidden_f * inv_rms * gain.astype(jnp.float32)).astype(jnp.bfloat16)


def rotary(values, positions):
    half_dim = values.shape[-1] // 2
    inv_freq = 500000.0 ** (-(jnp.arange(half_dim, dtype=jnp.float32) * 2.0 / values.shape[-1]))
    angles = positions.astype(jnp.float32)[:, None] * inv_freq[None, :]
    cos_ang = jnp.cos(angles)[:, None, :]
    sin_ang = jnp.sin(angles)[:, None, :]
    first = values[..., :half_dim]
    second = values[..., half_dim:]
    return jnp.concatenate([first * cos_ang - second * sin_ang, second * cos_ang + first * sin_ang], axis=-1)


def seg_positions(dev_ids, rows, dev_total):
    offset = jnp.arange(rows)
    half_len = rows // 2
    seg_idx = jnp.where(offset < half_len, dev_ids[..., None], 2 * dev_total - 1 - dev_ids[..., None])
    return seg_idx * half_len + offset % half_len


def attend(queries, keys_all, values_all, q_pos, k_pos, block_rows):
    rows, kv_loc, group, head_dim = queries.shape
    scale = 1.0 / math.sqrt(head_dim)
    q_blocks = queries.reshape(rows // block_rows, block_rows, kv_loc, group, head_dim)
    pos_blocks = q_pos.reshape(rows // block_rows, block_rows)

    def one_block(block):
        q_blk, pos_blk = block
        scores = jnp.einsum('bkgd,tkd->bkgt', q_blk, keys_all, preferred_element_type=jnp.float32) * scale
        visible = k_pos[None, None, None, :] <= pos_blk[:, None, None, None]
        scores = jnp.where(visible, scores, -jnp.inf)
        weights = jnp.exp(scores - jnp.max(scores, axis=-1, keepdims=True))
        row_sum = jnp.sum(weights, axis=-1, keepdims=True)
        mixed = jnp.einsum('bkgt,tkd->bkgd', weights.astype(jnp.bfloat16), values_all, preferred_element_type=jnp.float32)
        return (mixed / row_sum).astype(jnp.bfloat16)

    return lax.map(one_block, (q_blocks, pos_blocks)).reshape(rows, kv_loc * group, head_dim)


def solution(mesh):
    tp_size = mesh.shape['tp']
    cp_size = mesh.shape['cp']
    dev_total = tp_size * cp_size
    row_spec = P(('dp', 'tp', 'cp'), None)
    gain_spec = P(None, None)
    q_spec = P(None, None, 'tp', None)
    col_spec = P(None, None, 'tp')
    o_spec = P(None, 'tp', None, None)
    down_spec = P(None, 'tp', None)

    swap = [(i, (i + 1) % tp_size) for i in range(tp_size)]

    def body(tokens, norm_attn, norm_mlp, w_q, w_k, w_v, w_o, w_gate, w_up, w_down):
        rows = tokens.shape[0]
        heads_loc = w_q.shape[2]
        head_dim = w_q.shape[3]
        kv_loc = w_k.shape[2] // head_dim
        tp_idx = lax.axis_index('tp')
        cp_idx = lax.axis_index('cp')
        tp_devs = jnp.stack([tp_idx, 1 - tp_idx]) * cp_size + cp_idx
        pos_rows = seg_positions(tp_devs, rows, dev_total).reshape(tp_size * rows)
        hops = (cp_idx - jnp.arange(cp_size)) % cp_size
        key_devs = hops[:, None] + jnp.stack([tp_idx, 1 - tp_idx])[None, :] * cp_size
        pos_keys = seg_positions(key_devs, rows, dev_total).reshape(dev_total * rows)

        def ring(block):
            parts = [block]
            for hop in range(1, cp_size):
                parts.append(lax.ppermute(block, 'cp', [(i, (i + hop) % cp_size) for i in range(cp_size)]))
            return jnp.concatenate(parts, axis=0)

        hidden = tokens
        layers = w_q.shape[0]
        wq_flat = jnp.transpose(w_q, (0, 2, 3, 1)).reshape(layers, heads_loc * head_dim, w_q.shape[1])
        for layer_idx in range(layers):
            hidden_par = lax.ppermute(hidden, 'tp', swap)
            gain = norm_attn[layer_idx]
            normed = jnp.concatenate([rms_norm(hidden, gain), rms_norm(hidden_par, gain)], axis=0)
            q_proj = lax.dot_general(normed, wq_flat[layer_idx], (((1,), (1,)), ((), ())), preferred_element_type=jnp.float32)
            queries = rotary(q_proj.reshape(tp_size * rows, heads_loc, head_dim), pos_rows).astype(jnp.bfloat16)
            k_proj = jnp.dot(normed, w_k[layer_idx], preferred_element_type=jnp.float32)
            keys_loc = rotary(k_proj.reshape(tp_size * rows, kv_loc, head_dim), pos_rows).astype(jnp.bfloat16)
            values_loc = jnp.dot(normed, w_v[layer_idx], preferred_element_type=jnp.float32).astype(jnp.bfloat16)
            kv = ring(jnp.concatenate([keys_loc.reshape(tp_size * rows, kv_loc * head_dim), values_loc], axis=1))
            keys_all = kv[:, :kv_loc * head_dim].reshape(dev_total * rows, kv_loc, head_dim)
            values_all = kv[:, kv_loc * head_dim:].reshape(dev_total * rows, kv_loc, head_dim)
            grouped = queries.reshape(tp_size * rows, kv_loc, heads_loc // kv_loc, head_dim)
            mixed = attend(grouped, keys_all, values_all, pos_rows, pos_keys, rows).reshape(tp_size * rows, heads_loc * head_dim)
            wo = w_o[layer_idx].reshape(heads_loc * head_dim, w_o.shape[3])
            part_par = jnp.dot(mixed[rows:], wo, preferred_element_type=jnp.float32)
            got = lax.ppermute(part_par, 'tp', swap)
            part_own = jnp.dot(mixed[:rows], wo, preferred_element_type=jnp.float32)
            hidden_mid = (hidden.astype(jnp.float32) + (part_own + got)).astype(jnp.bfloat16)
            mid_par = lax.ppermute(hidden_mid, 'tp', swap)
            gain = norm_mlp[layer_idx]

            def mlp_act(rows_in):
                normed_mlp = rms_norm(rows_in, gain)
                gate_pre = jnp.dot(normed_mlp, w_gate[layer_idx], preferred_element_type=jnp.float32)
                up_proj = jnp.dot(normed_mlp, w_up[layer_idx], preferred_element_type=jnp.float32)
                return (jax.nn.silu(gate_pre) * up_proj).astype(jnp.bfloat16)

            act = mlp_act(jnp.concatenate([hidden_mid, mid_par], axis=0))
            down_par = jnp.dot(act[rows:], w_down[layer_idx], preferred_element_type=jnp.float32)
            got = lax.ppermute(down_par, 'tp', swap)
            down_own = jnp.dot(act[:rows], w_down[layer_idx], preferred_element_type=jnp.float32)
            hidden = (hidden_mid.astype(jnp.float32) + (down_own + got)).astype(jnp.bfloat16)
        return hidden

    return jax.shard_map(
        body,
        mesh=mesh,
        in_specs=(row_spec, gain_spec, gain_spec, q_spec, col_spec, col_spec, o_spec, col_spec, col_spec, down_spec),
        out_specs=row_spec,
        check_vma=False,
    )
```

```python
import functools
import math

import jax
import jax.numpy as jnp
from jax import lax
from jax.experimental import pallas as pl
from jax.experimental.pallas import tpu as pltpu
from jax.sharding import PartitionSpec as P

MESH = pl.DeviceIdType.MESH
F32 = jnp.float32
BF16 = jnp.bfloat16
ROWS, SEG, D, HEAD, FF = 128, 64, 2048, 64, 4096
CH, NCH = 256, 8
GCH, NGC = 512, 8
RING = 4
LAYERS = 2
EXP2_SCALE = math.log2(math.e) / math.sqrt(HEAD)


def kernel(tokens, gain_attn, gain_mlp, cos_ref, sin_ref, wq, wk, wv, wo, wg, wu, wd, out,
           x_own, x_par, a_ref, qh, o_ref, kv, act, sbuf, rbuf, slot, wk_v, wv_v, wg_v, wu_v, wd_v,
           tok_sem, out_sem, slot_sem, kvw_sem, gu_sem, wd_sem, xs_sem, xr_sem, ps_sem, pr_sem, ks_sem, kr_sem):
    t = lax.axis_index('tp')
    c = lax.axis_index('cp')
    other = {'tp': 1 - t}

    def load_slot(src):
        return [pltpu.make_async_copy(src.at[pl.ds(i * 512, 512)], slot.at[pl.ds(i * 512, 512)], slot_sem.at[i]) for i in range(2)]

    def load_kvw(l):
        return [pltpu.make_async_copy(wk.at[l], wk_v, kvw_sem.at[0]), pltpu.make_async_copy(wv.at[l], wv_v, kvw_sem.at[1])]

    def load_gu(l, j):
        cols = pl.ds(pl.multiple_of(j * GCH, GCH), GCH)
        return [pltpu.make_async_copy(wg.at[l, :, cols], wg_v.at[j], gu_sem.at[0, j]),
                pltpu.make_async_copy(wu.at[l, :, cols], wu_v.at[j], gu_sem.at[1, j])]

    def load_wd(l, j):
        cols = pl.ds(pl.multiple_of(j * CH, CH), CH)
        s = lax.rem(j, RING)
        return pltpu.make_async_copy(wd.at[l, :, cols], wd_v.at[s], wd_sem.at[s])

    def start(copies):
        for copy in copies:
            copy.start()

    def wait(copies):
        for copy in copies:
            copy.wait()

    def send_x(src, j):
        return pltpu.make_async_remote_copy(src, x_par.at[j], xs_sem.at[j], xr_sem.at[j], other, MESH)

    def send_part(j):
        return pltpu.make_async_remote_copy(sbuf.at[j], rbuf.at[j], ps_sem.at[j], pr_sem.at[j], other, MESH)

    def segments(g, ti, ci):
        k = (ti if g == 0 else 1 - ti) * 4 + ci
        return k, 15 - k

    def send_kv(l, hop, g, i, ci):
        rows = pl.ds(pl.multiple_of(segments(g, t, ci)[i] * SEG, SEG), SEG)
        place = kv.at[l, rows, :]
        return pltpu.make_async_remote_copy(place, place, ks_sem.at[l, hop, g, i], kr_sem.at[l, hop, g, i],
                                            {'cp': lax.rem(c + hop + 1, 4)}, MESH)

    tok = [pltpu.make_async_copy(tokens.at[:, pl.ds(j * CH, CH)], x_own.at[j], tok_sem.at[j]) for j in range(NCH)]
    start(tok)
    start(load_kvw(0))
    start(load_slot(wq.at[0]))

    barrier = pltpu.get_barrier_semaphore()
    pl.semaphore_signal(barrier, inc=1, device_id=other, device_id_type=MESH)
    for hop in range(3):
        pl.semaphore_signal(barrier, inc=1, device_id={'cp': lax.rem(c + hop + 1, 4)}, device_id_type=MESH)
    pl.semaphore_wait(barrier, 4)
    for j in range(NCH):
        send_x(tokens.at[:, pl.ds(j * CH, CH)], j).start()
    for j in range(NGC):
        start(load_gu(0, j))
    for j in range(RING):
        load_wd(0, j).start()

    lane = lax.broadcasted_iota(jnp.int32, (ROWS, 128), 1)
    first_half = (lane % HEAD) < HEAD // 2
    low = lane < HEAD
    low_seg = lax.broadcasted_iota(jnp.int32, (SEG, 128), 1) < HEAD
    diff = (lax.broadcasted_iota(jnp.int32, (4 * SEG, 512), 1)
            - lax.broadcasted_iota(jnp.int32, (4 * SEG, 512), 0) % SEG)

    def norm(x_ref, gain, g):
        total = jnp.zeros((ROWS, 1), F32)
        for j in range(NCH):
            x = x_ref[j].astype(F32)
            total = total + jnp.sum(x * x, axis=-1, keepdims=True)
        inv = lax.rsqrt(total * (1.0 / D) + 1e-5)
        for j in range(NCH):
            cols = pl.ds(j * CH, CH)
            a_ref[g, :, cols] = (x_ref[j].astype(F32) * inv * gain[:, cols]).astype(BF16)

    def rope(v, g):
        swapped = jnp.where(first_half, pltpu.roll(v, 128 - HEAD // 2, 1), pltpu.roll(v, HEAD // 2, 1))
        return v * cos_ref[g] + swapped * sin_ref[g]

    def qkv(l, g):
        k_new = jnp.dot(a_ref[g], wk_v[...], preferred_element_type=F32)
        v_new = jnp.dot(a_ref[g], wv_v[...], preferred_element_type=F32).astype(BF16)
        k_new = jnp.concatenate([rope(k_new[:, :128], g), rope(k_new[:, 128:], g)], axis=1).astype(BF16)
        for i in range(2):
            rows = pl.ds(pl.multiple_of(segments(g, t, c)[i] * SEG, SEG), SEG)
            kv[l, rows, 0:256] = k_new[i * SEG:(i + 1) * SEG]
            kv[l, rows, 256:512] = v_new[i * SEG:(i + 1) * SEG]
        for i in range(2):
            for hop in (1, 0, 2):
                send_kv(l, hop, g, i, c).start()
        for h in range(4):
            q = lax.dot_general(a_ref[g], slot[h * 256:(h + 1) * 256, :], (((1,), (1,)), ((), ())), preferred_element_type=F32)
            for pair in range(2):
                both = rope(q[:, pair * 128:(pair + 1) * 128], g)
                turned = pltpu.roll(both, HEAD, 1)
                for odd in range(2):
                    value = both if odd == h % 2 else turned
                    value = jnp.where(low if h % 2 == 0 else ~low, value, 0.0).astype(BF16)
                    n = pair * 2 + odd
                    for i in range(2):
                        qh[g, i, h, n * SEG:(n + 1) * SEG, :] = value[i * SEG:(i + 1) * SEG]

    def attention(l, g):
        for i in range(2):
            seg = segments(g, t, c)[i]
            free = 512 * i
            visible = diff <= seg * SEG - free
            for parity in range(2):
                def pair_step(p, carry, i=i, free=free, visible=visible, parity=parity):
                    h = 2 * p + parity
                    k_cols = pl.ds(pl.multiple_of(p * 128, 128), 128)
                    v_cols = pl.ds(pl.multiple_of(256 + p * 128, 128), 128)
                    q = qh[g, i, h]
                    nt = (((1,), (1,)), ((), ()))
                    s_end = lax.dot_general(q, kv[l, pl.ds(free, 512), k_cols], nt, preferred_element_type=F32)
                    s_end = jnp.where(visible, s_end, -jnp.inf)
                    top = jnp.max(s_end, axis=-1, keepdims=True)
                    if free:
                        s_free = lax.dot_general(q, kv[l, pl.ds(0, free), k_cols], nt, preferred_element_type=F32)
                        top = jnp.maximum(top, jnp.max(s_free, axis=-1, keepdims=True))
                    e_end = jnp.exp2((s_end - top) * EXP2_SCALE)
                    total = jnp.sum(e_end, axis=-1, keepdims=True)
                    mixed = jnp.dot(e_end.astype(BF16), kv[l, pl.ds(free, 512), v_cols], preferred_element_type=F32)
                    if free:
                        e_free = jnp.exp2((s_free - top) * EXP2_SCALE)
                        total = total + jnp.sum(e_free, axis=-1, keepdims=True)
                        mixed = mixed + jnp.dot(e_free.astype(BF16), kv[l, pl.ds(0, free), v_cols], preferred_element_type=F32)
                    mixed = mixed / total
                    for pair in range(2):
                        sides = []
                        for odd in range(2):
                            n = pair * 2 + odd
                            value = mixed[n * SEG:(n + 1) * SEG]
                            sides.append(value if odd == parity else pltpu.roll(value, HEAD, 1))
                        cols = pl.ds(pl.multiple_of(h * 256 + pair * 128, 128), 128)
                        o_ref[g, i * SEG:(i + 1) * SEG, cols] = jnp.where(low_seg, sides[0], sides[1]).astype(BF16)
                    return carry
                lax.fori_loop(0, 2, pair_step, 0)

    def slot_chunk(lhs, j):
        return jnp.dot(lhs, slot[:, pl.ds(pl.multiple_of(j * CH, CH), CH)], preferred_element_type=F32)

    def reduce_chunk(own, j):
        send_part(j).wait_recv()
        return (x_own[j].astype(F32) + (own + rbuf[j])).astype(BF16)

    for l in range(LAYERS):
        last = l == LAYERS - 1
        if l == 0:
            wait(tok)
        norm(x_own, gain_attn[l], 0)
        wait(load_kvw(l))
        wait(load_slot(wq.at[l]))
        qkv(l, 0)
        for j in range(NCH):
            send_x(x_own.at[j], j).wait_recv()
        norm(x_par, gain_attn[l], 1)
        qkv(l, 1)
        start(load_slot(wo.at[l]))
        if not last:
            start(load_kvw(l + 1))
        for g in range(2):
            for i in range(2):
                for hop in range(3):
                    send_kv(l, hop, g, i, lax.rem(c + 3 - hop, 4)).wait_recv()
        attention(l, 1)
        wait(load_slot(wo.at[l]))

        def o_send(j, carry, l=l):
            part = slot_chunk(o_ref[1], j)
            if l > 0:
                send_part(j).wait_send()
            sbuf[j] = part
            send_part(j).start()
            return carry
        lax.fori_loop(0, NCH, o_send, 0)
        attention(l, 0)

        def o_reduce(j, carry):
            new = reduce_chunk(slot_chunk(o_ref[0], j), j)
            send_x(x_own.at[j], j).wait_send()
            x_own[j] = new
            send_x(x_own.at[j], j).start()
            return carry
        lax.fori_loop(0, NCH, o_reduce, 0)
        if not last:
            start(load_slot(wq.at[l + 1]))

        def gate_up(g, l=l, last=last):
            def step(j, carry):
                if g == 0:
                    wait(load_gu(l, j))
                gate = jnp.dot(a_ref[g], wg_v[j], preferred_element_type=F32)
                up = jnp.dot(a_ref[g], wu_v[j], preferred_element_type=F32)
                act[g, :, pl.ds(pl.multiple_of(j * GCH, GCH), GCH)] = (gate * jax.nn.sigmoid(gate) * up).astype(BF16)
                if g == 1 and not last:
                    start(load_gu(l + 1, j))
                return carry
            lax.fori_loop(0, NGC, step, 0)

        norm(x_own, gain_mlp[l], 0)
        gate_up(0)
        for j in range(NCH):
            send_x(x_own.at[j], j).wait_recv()
        norm(x_par, gain_mlp[l], 1)
        gate_up(1)

        def down_chunk(g, j, l=l):
            load_wd(l, j).wait()
            return jnp.dot(act[g], wd_v[lax.rem(j, RING)], preferred_element_type=F32)

        def down_send(j, carry, l=l):
            part = down_chunk(1, j)
            load_wd(l, lax.rem(j + RING, NCH)).start()
            send_part(j).wait_send()
            sbuf[j] = part
            send_part(j).start()
            return carry
        lax.fori_loop(0, NCH, down_send, 0)

        def down_reduce(j, carry, l=l, last=last):
            own = down_chunk(0, j)
            if last:
                @pl.when(j < NCH - RING)
                def _():
                    load_wd(l, j + RING).start()
            else:
                @pl.when(j < NCH - RING)
                def _():
                    load_wd(l, j + RING).start()

                @pl.when(j >= NCH - RING)
                def _():
                    load_wd(l + 1, j + RING - NCH).start()
            new = reduce_chunk(own, j)
            send_x(x_own.at[j], j).wait_send()
            x_own[j] = new
            cols = pl.ds(pl.multiple_of(j * CH, CH), CH)
            if last:
                pltpu.make_async_copy(x_own.at[j], out.at[:, cols], out_sem.at[j]).start()
            else:
                send_x(x_own.at[j], j).start()
            return carry
        lax.fori_loop(0, NCH, down_reduce, 0)

    for j in range(NCH):
        send_part(j).wait_send()
        pltpu.make_async_copy(x_own.at[j], out.at[:, pl.ds(j * CH, CH)], out_sem.at[j]).wait()
    for l in range(LAYERS):
        for g in range(2):
            for i in range(2):
                for hop in range(3):
                    send_kv(l, hop, g, i, c).wait_send()


def solution(mesh):
    tp_size = mesh.shape['tp']
    cp_size = mesh.shape['cp']
    row_spec = P(('dp', 'tp', 'cp'), None)
    gain_spec = P(None, None)
    q_spec = P(None, None, 'tp', None)
    col_spec = P(None, None, 'tp')
    o_spec = P(None, 'tp', None, None)
    down_spec = P(None, 'tp', None)

    def body(tokens, norm_attn, norm_mlp, w_q, w_k, w_v, w_o, w_gate, w_up, w_down):
        t = lax.axis_index('tp')
        c = lax.axis_index('cp')
        dev = jnp.stack([t, 1 - t]) * cp_size + c
        seg = jnp.stack([dev, 2 * tp_size * cp_size - 1 - dev], axis=1)
        pos = (seg[:, :, None] * SEG + jnp.arange(SEG)[None, None, :]).reshape(2, ROWS)
        inv_freq = 500000.0 ** (-(jnp.arange(HEAD // 2, dtype=F32) * 2.0 / HEAD))
        angles = pos.astype(F32)[:, :, None] * inv_freq
        cos, sin = jnp.cos(angles), jnp.sin(angles)
        cos = jnp.concatenate([cos, cos, cos, cos], axis=-1)
        sin = jnp.concatenate([-sin, sin, -sin, sin], axis=-1)
        wq = jnp.transpose(w_q, (0, 2, 3, 1)).reshape(LAYERS, 1024, D)
        wo = w_o.reshape(LAYERS, 1024, D)
        hbm = pl.BlockSpec(memory_space=pl.ANY)
        vmem = pl.BlockSpec(memory_space=pltpu.VMEM)
        dma = pltpu.SemaphoreType.DMA
        return pl.pallas_call(
            kernel,
            out_shape=jax.ShapeDtypeStruct((ROWS, D), BF16),
            in_specs=[hbm, vmem, vmem, vmem, vmem] + [hbm] * 7,
            out_specs=hbm,
            scratch_shapes=[
                pltpu.VMEM((NCH, ROWS, CH), BF16),
                pltpu.VMEM((NCH, ROWS, CH), BF16),
                pltpu.VMEM((2, ROWS, D), BF16),
                pltpu.VMEM((2, 2, 4, 4 * SEG, 128), BF16),
                pltpu.VMEM((2, ROWS, 1024), BF16),
                pltpu.VMEM((LAYERS, 1024, 512), BF16),
                pltpu.VMEM((2, ROWS, FF), BF16),
                pltpu.VMEM((NCH, ROWS, CH), F32),
                pltpu.VMEM((NCH, ROWS, CH), F32),
                pltpu.VMEM((1024, D), BF16),
                pltpu.VMEM((D, 256), BF16),
                pltpu.VMEM((D, 256), BF16),
                pltpu.VMEM((NGC, D, GCH), BF16),
                pltpu.VMEM((NGC, D, GCH), BF16),
                pltpu.VMEM((RING, FF, CH), BF16),
                dma((NCH,)), dma((NCH,)), dma((2,)), dma((2,)), dma((2, NGC)), dma((RING,)),
                dma((NCH,)), dma((NCH,)), dma((NCH,)), dma((NCH,)),
                dma((LAYERS, 3, 2, 2)), dma((LAYERS, 3, 2, 2)),
            ],
            compiler_params=pltpu.CompilerParams(
                collective_id=0, has_side_effects=True, vmem_limit_bytes=67_000_000),
            name='decoder',
        )(tokens, norm_attn.astype(F32).reshape(LAYERS, 1, D), norm_mlp.astype(F32).reshape(LAYERS, 1, D), cos, sin,
          wq, w_k, w_v, wo, w_gate, w_up, w_down)

    return jax.shard_map(
        body,
        mesh=mesh,
        in_specs=(row_spec, gain_spec, gain_spec, q_spec, col_spec, col_spec, o_spec, col_spec, col_spec, down_spec),
        out_specs=row_spec,
        check_vma=False,
    )
```

```python
import math

import jax
import jax.numpy as jnp
import numpy as np
from jax import lax
from jax.experimental import pallas as pl
from jax.experimental.pallas import tpu as pltpu
from jax.sharding import PartitionSpec as P

MESH = pl.DeviceIdType.MESH
F32 = jnp.float32
BF16 = jnp.bfloat16
ROWS, SEG, D, HEAD, FF = 128, 64, 2048, 64, 4096
CH, NCH = 256, 8
GCH, NGC = 512, 8
RING = 4
PIECES, PIECE = 8, 32
FIRST, MIDDLE, LATE = (0, 1, 2, 3), (4, 5), (6, 7)
LAYERS = 2
EXP2_SCALE = math.log2(math.e) / math.sqrt(HEAD)


def kernel(tokens, gain_attn, gain_mlp, table, wq, wk, wv, wo, wg, wu, wd, out,
           x_own, x_par, a_ref, qh, o_ref, o_x, kv, act, sbuf, rbuf, slot, wo_x, wk_v, wv_v, wg_v, wu_v, wd_v,
           turns, cos_ref, sin_ref,
           tok_sem, out_sem, slot_sem, kvw_sem, gu_sem, wd_sem, turn_sem, xs_sem, xr_sem, ps_sem, pr_sem, ds_sem, dr_sem,
           ks_sem, kr_sem, os_sem, or_sem, ws_sem, wr_sem, fs_sem, fr_sem):
    t = lax.axis_index('tp')
    c = lax.axis_index('cp')
    other = {'tp': 1 - t}
    beside, across, corner = c + 1 - 2 * lax.rem(c, 2), lax.rem(c + 2, 4), 3 - c
    peers = (beside, across, corner)

    def load_slot(src):
        return [pltpu.make_async_copy(src.at[pl.ds(i * 512, 512)], slot.at[pl.ds(i * 512, 512)], slot_sem.at[i]) for i in range(2)]

    def load_kvw(l):
        return [pltpu.make_async_copy(wk.at[l], wk_v, kvw_sem.at[0]), pltpu.make_async_copy(wv.at[l], wv_v, kvw_sem.at[1])]

    def load_gu(l, j):
        cols = pl.ds(pl.multiple_of(j * GCH, GCH), GCH)
        return [pltpu.make_async_copy(wg.at[l, :, cols], wg_v.at[j], gu_sem.at[0, j]),
                pltpu.make_async_copy(wu.at[l, :, cols], wu_v.at[j], gu_sem.at[1, j])]

    def load_wd(l, j):
        cols = pl.ds(pl.multiple_of(j * CH, CH), CH)
        s = lax.rem(j, RING)
        return pltpu.make_async_copy(wd.at[l, :, cols], wd_v.at[s], wd_sem.at[s])

    def start(copies):
        for copy in copies:
            copy.start()

    def wait(copies):
        for copy in copies:
            copy.wait()

    def send_x(src, j):
        return pltpu.make_async_remote_copy(src, x_par.at[j], xs_sem.at[j], xr_sem.at[j], other, MESH)

    def send_part(j):
        return pltpu.make_async_remote_copy(sbuf.at[j], rbuf.at[j], ps_sem.at[j], pr_sem.at[j], other, MESH)

    def segments(g, ti, ci):
        k = (ti if g == 0 else 1 - ti) * 4 + ci
        return k, 15 - k

    def send_half(i, j):
        place = (j, pl.ds(i * SEG, SEG))
        return pltpu.make_async_remote_copy(sbuf.at[place], rbuf.at[place], ds_sem.at[i, j], dr_sem.at[i, j], other, MESH)

    def send_o(g):
        return pltpu.make_async_remote_copy(o_ref.at[g], o_x.at[1 - g], os_sem.at[g], or_sem.at[1 - g], other, MESH)

    def recv_o(g):
        return pltpu.make_async_remote_copy(o_ref.at[g], o_x.at[g], os_sem.at[g], or_sem.at[g], other, MESH)

    def send_kv(l, kind, g, i, owner, to):
        rows = pl.ds(pl.multiple_of(segments(g, t, owner)[i] * SEG, SEG), SEG)
        place = kv.at[l, rows, :]
        return pltpu.make_async_remote_copy(place, place, ks_sem.at[l, kind, g, i], kr_sem.at[l, kind, g, i], {'cp': to}, MESH)

    def piece(owner, p):
        return pl.ds(pl.multiple_of(owner * (PIECES * PIECE) + p * PIECE, PIECE), PIECE)

    def send_wo(p):
        return pltpu.make_async_remote_copy(wo.at[1, piece(c, p)], wo_x.at[piece(c, p)], ws_sem.at[p], wr_sem.at[p], other, MESH)

    def spread_wo(kind, p, owner, to):
        place = wo_x.at[piece(owner, p)]
        return pltpu.make_async_remote_copy(place, place, fs_sem.at[kind, p], fr_sem.at[kind, p], {'cp': to}, MESH)

    def pass_wo(pieces):
        for p in pieces:
            send_wo(p).wait_recv()
            spread_wo(1, p, c, across).start()
            spread_wo(0, p, c, beside).start()

    def relay_wo(pieces):
        for p in pieces:
            spread_wo(1, p, across, across).wait_recv()
            spread_wo(2, p, across, beside).start()

    tok = [pltpu.make_async_copy(tokens.at[:, pl.ds(j * CH, CH)], x_own.at[j], tok_sem.at[j]) for j in range(NCH)]
    start(tok)
    turn = [pltpu.make_async_copy(table.at[pl.ds(pl.multiple_of(segments(g, t, c)[i] * SEG, SEG), SEG)],
                                  turns.at[g, pl.ds(i * SEG, SEG)], turn_sem.at[g, i]) for g in range(2) for i in range(2)]
    start(turn)
    start(load_kvw(0))
    start(load_slot(wq.at[0]))

    barrier = pltpu.get_barrier_semaphore()
    pl.semaphore_signal(barrier, inc=1, device_id=other, device_id_type=MESH)
    for to in peers:
        pl.semaphore_signal(barrier, inc=1, device_id={'cp': to}, device_id_type=MESH)
    pl.semaphore_wait(barrier, 4)
    for j in range(NCH):
        send_x(tokens.at[:, pl.ds(j * CH, CH)], j).start()
    for j in range(NGC):
        start(load_gu(0, j))
    for j in range(RING):
        load_wd(0, j).start()

    lane = lax.broadcasted_iota(jnp.int32, (ROWS, 128), 1)
    first_half = (lane % HEAD) < HEAD // 2
    low = lane < HEAD
    low_seg = lax.broadcasted_iota(jnp.int32, (SEG, 128), 1) < HEAD
    diff = (lax.broadcasted_iota(jnp.int32, (4 * SEG, 512), 1)
            - lax.broadcasted_iota(jnp.int32, (4 * SEG, 512), 0) % SEG)

    wait(turn)
    for g in range(2):
        near, far = turns[g], pltpu.roll(turns[g], HEAD, 1)
        cos_ref[g] = jnp.where(low, near, far)
        sin_ref[g] = jnp.where(low, far, near)

    def norm(x_ref, gain_ref, l):
        total = jnp.zeros((ROWS, 1), F32)
        for j in range(NCH):
            x = x_ref[j].astype(F32)
            total = total + jnp.sum(x * x, axis=-1, keepdims=True)
        inv = lax.rsqrt(total * (1.0 / D) + 1e-5)
        for j in range(NCH):
            cols = pl.ds(j * CH, CH)
            a_ref[:, cols] = (x_ref[j].astype(F32) * inv * gain_ref[l:l + 1, cols].astype(F32)).astype(BF16)

    def rope(v, g):
        swapped = jnp.where(first_half, pltpu.roll(v, 128 - HEAD // 2, 1), pltpu.roll(v, HEAD // 2, 1))
        return v * cos_ref[g] + swapped * sin_ref[g]

    def qkv(l, g):
        k_new = jnp.dot(a_ref[...], wk_v[...], preferred_element_type=F32)
        v_new = jnp.dot(a_ref[...], wv_v[...], preferred_element_type=F32).astype(BF16)
        k_new = jnp.concatenate([rope(k_new[:, :128], g), rope(k_new[:, 128:], g)], axis=1).astype(BF16)
        for i in range(2):
            rows = pl.ds(pl.multiple_of(segments(g, t, c)[i] * SEG, SEG), SEG)
            kv[l, rows, 0:256] = k_new[i * SEG:(i + 1) * SEG]
            kv[l, rows, 256:512] = v_new[i * SEG:(i + 1) * SEG]
        for i in range(2):
            for kind in ((1, 2, 0) if g == 0 else (1, 0)):
                send_kv(l, kind, g, i, c, peers[kind]).start()
        for h in range(4):
            q = lax.dot_general(a_ref[...], slot[h * 256:(h + 1) * 256, :], (((1,), (1,)), ((), ())), preferred_element_type=F32)
            for pair in range(2):
                both = rope(q[:, pair * 128:(pair + 1) * 128], g)
                turned = pltpu.roll(both, HEAD, 1)
                for odd in range(2):
                    value = both if odd == h % 2 else turned
                    value = jnp.where(low if h % 2 == 0 else ~low, value, 0.0).astype(BF16)
                    n = pair * 2 + odd
                    for i in range(2):
                        qh[g, i, h, n * SEG:(n + 1) * SEG, :] = value[i * SEG:(i + 1) * SEG]

    def attention(l, g, parts=(0, 1)):
        for i in parts:
            seg = segments(g, t, c)[i]
            free = 512 * i
            visible = diff <= seg * SEG - free
            for parity in range(2):
                def pair_step(p, carry, i=i, free=free, visible=visible, parity=parity):
                    h = 2 * p + parity
                    k_cols = pl.ds(pl.multiple_of(p * 128, 128), 128)
                    v_cols = pl.ds(pl.multiple_of(256 + p * 128, 128), 128)
                    q = qh[g, i, h]
                    nt = (((1,), (1,)), ((), ()))
                    s_end = lax.dot_general(q, kv[l, pl.ds(free, 512), k_cols], nt, preferred_element_type=F32)
                    s_end = jnp.where(visible, s_end, -jnp.inf)
                    top = jnp.max(s_end, axis=-1, keepdims=True)
                    if free:
                        s_free = lax.dot_general(q, kv[l, pl.ds(0, free), k_cols], nt, preferred_element_type=F32)
                        top = jnp.maximum(top, jnp.max(s_free, axis=-1, keepdims=True))
                    e_end = jnp.exp2((s_end - top) * EXP2_SCALE)
                    total = jnp.sum(e_end, axis=-1, keepdims=True)
                    mixed = jnp.dot(e_end.astype(BF16), kv[l, pl.ds(free, 512), v_cols], preferred_element_type=F32)
                    if free:
                        e_free = jnp.exp2((s_free - top) * EXP2_SCALE)
                        total = total + jnp.sum(e_free, axis=-1, keepdims=True)
                        mixed = mixed + jnp.dot(e_free.astype(BF16), kv[l, pl.ds(0, free), v_cols], preferred_element_type=F32)
                    mixed = mixed / total
                    for pair in range(2):
                        sides = []
                        for odd in range(2):
                            n = pair * 2 + odd
                            value = mixed[n * SEG:(n + 1) * SEG]
                            sides.append(value if odd == parity else pltpu.roll(value, HEAD, 1))
                        cols = pl.ds(pl.multiple_of(h * 256 + pair * 128, 128), 128)
                        o_ref[g, i * SEG:(i + 1) * SEG, cols] = jnp.where(low_seg, sides[0], sides[1]).astype(BF16)
                    return carry
                lax.fori_loop(0, 2, pair_step, 0)

    def slot_chunk(lhs, j):
        return jnp.dot(lhs, slot[:, pl.ds(pl.multiple_of(j * CH, CH), CH)], preferred_element_type=F32)

    def reduce_chunk(own, j):
        return (x_own[j].astype(F32) + (own + rbuf[j])).astype(BF16)

    for l in range(LAYERS):
        last = l == LAYERS - 1
        if l == 0:
            wait(tok)
        norm(x_own, gain_attn, l)
        wait(load_kvw(l))
        wait(load_slot(wq.at[l]))
        qkv(l, 0)
        for j in range(NCH):
            send_x(x_own.at[j], j).wait_recv()
        norm(x_par, gain_attn, l)
        qkv(l, 1)
        start(load_slot(wo.at[l]))
        if not last:
            start(load_kvw(l + 1))
        for p in FIRST if not last else LATE:
            send_wo(p).start()
        for i in range(2):
            send_kv(l, 1, 1, i, across, across).wait_recv()
            send_kv(l, 2, 1, i, across, beside).start()
        for g in range(2):
            for i in range(2):
                for kind in range(3):
                    if (kind, g) != (1, 1):
                        send_kv(l, kind, g, i, peers[kind], peers[kind]).wait_recv()

        if not last:
            wait(load_slot(wo.at[l]))
            for i in range(2):
                attention(l, 1, (i,))

                def o_send(j, carry, i=i):
                    rows = pl.ds(i * SEG, SEG)
                    sbuf[j, rows] = slot_chunk(o_ref[1, rows], j)
                    send_half(i, j).start()
                    return carry
                lax.fori_loop(0, NCH, o_send, 0)
            pass_wo(FIRST)
            attention(l, 0)

            def o_reduce(j, carry):
                own = slot_chunk(o_ref[0], j)
                send_half(0, j).wait_recv()
                send_half(1, j).wait_recv()
                new = reduce_chunk(own, j)
                send_x(x_own.at[j], j).wait_send()
                x_own[j] = new
                send_x(x_own.at[j], j).start()
                return carry
            lax.fori_loop(0, NCH, o_reduce, 0)
            relay_wo(FIRST)
            start(load_slot(wq.at[l + 1]))
        else:
            pass_wo(LATE)
            attention(l, 0)
            send_o(0).start()
            attention(l, 1)
            send_o(1).start()
            relay_wo(LATE)
            wait(load_slot(wo.at[l]))

            def o_near(j, carry):
                send_part(j).wait_send()
                sbuf[j] = slot_chunk(o_ref[1], j)
                return carry
            lax.fori_loop(0, NCH, o_near, 0)
            for p in range(PIECES):
                spread_wo(0, p, beside, beside).wait_recv()
                spread_wo(2, p, corner, beside).wait_recv()

        def gate_up(g, l=l, last=last):
            def step(j, carry):
                if g == (1 if last else 0):
                    wait(load_gu(l, j))
                gate = jnp.dot(a_ref[...], wg_v[j], preferred_element_type=F32)
                up = jnp.dot(a_ref[...], wu_v[j], preferred_element_type=F32)
                act[g, :, pl.ds(pl.multiple_of(j * GCH, GCH), GCH)] = (gate * jax.nn.sigmoid(gate) * up).astype(BF16)
                if g == 1 and not last:
                    start(load_gu(l + 1, j))
                return carry
            lax.fori_loop(0, NGC, step, 0)

        def far_chunk(g, j):
            return jnp.dot(o_x[g], wo_x[:, pl.ds(pl.multiple_of(j * CH, CH), CH)], preferred_element_type=F32)

        if not last:
            norm(x_own, gain_mlp, l)
            gate_up(0)
            for j in range(NCH):
                send_x(x_own.at[j], j).wait_recv()
            for p in MIDDLE:
                send_wo(p).start()
            norm(x_par, gain_mlp, l)
            gate_up(1)
        else:
            recv_o(1).wait_recv()

            def o_far(j, carry):
                x_par[j] = (x_par[j].astype(F32) + (sbuf[j] + far_chunk(1, j))).astype(BF16)
                return carry
            lax.fori_loop(0, NCH, o_far, 0)
            norm(x_par, gain_mlp, l)
            gate_up(1)

        def down_chunk(g, j, l=l):
            load_wd(l, j).wait()
            return jnp.dot(act[g], wd_v[lax.rem(j, RING)], preferred_element_type=F32)

        def down_send(j, carry, l=l, last=last):
            part = down_chunk(1, j)
            load_wd(l, lax.rem(j + RING, NCH)).start()
            if not last:
                send_half(0, j).wait_send()
                send_half(1, j).wait_send()
            sbuf[j] = part
            send_part(j).start()
            return carry
        lax.fori_loop(0, NCH, down_send, 0)
        if not last:
            pass_wo(MIDDLE)
        else:
            recv_o(0).wait_recv()

            def o_own(j, carry):
                new = (x_own[j].astype(F32) + (slot_chunk(o_ref[0], j) + far_chunk(0, j))).astype(BF16)
                send_x(x_own.at[j], j).wait_send()
                x_own[j] = new
                return carry
            lax.fori_loop(0, NCH, o_own, 0)
            norm(x_own, gain_mlp, l)
            gate_up(0)

        def down_reduce(j, carry, l=l, last=last):
            own = down_chunk(0, j)
            if last:
                @pl.when(j < NCH - RING)
                def _():
                    load_wd(l, j + RING).start()
            else:
                @pl.when(j < NCH - RING)
                def _():
                    load_wd(l, j + RING).start()

                @pl.when(j >= NCH - RING)
                def _():
                    load_wd(l + 1, j + RING - NCH).start()
            send_part(j).wait_recv()
            new = reduce_chunk(own, j)
            if not last:
                send_x(x_own.at[j], j).wait_send()
            x_own[j] = new
            cols = pl.ds(pl.multiple_of(j * CH, CH), CH)
            if last:
                pltpu.make_async_copy(x_own.at[j], out.at[:, cols], out_sem.at[j]).start()
            else:
                send_x(x_own.at[j], j).start()
            return carry
        lax.fori_loop(0, NCH, down_reduce, 0)
        if not last:
            relay_wo(MIDDLE)

    for j in range(NCH):
        send_part(j).wait_send()
        pltpu.make_async_copy(x_own.at[j], out.at[:, pl.ds(j * CH, CH)], out_sem.at[j]).wait()
    for l in range(LAYERS):
        for g in range(2):
            for i in range(2):
                for kind in range(3):
                    send_kv(l, kind, g, i, c, beside).wait_send()
    for g in range(2):
        send_o(g).wait_send()
    for p in range(PIECES):
        send_wo(p).wait_send()
        for kind in range(3):
            spread_wo(kind, p, c, beside).wait_send()


def turn_table():
    inv_freq = np.float32(500000.0) ** (-(np.arange(HEAD // 2, dtype=np.float32) * np.float32(2.0) / np.float32(HEAD)))
    angles = np.arange(16 * SEG, dtype=np.float32)[:, None] * inv_freq.astype(np.float32)[None, :]
    cos, sin = np.cos(angles), np.sin(angles)
    return np.concatenate([cos, cos, -sin, sin], axis=1).astype(np.float32)


def solution(mesh):
    tp_size = mesh.shape['tp']
    cp_size = mesh.shape['cp']
    row_spec = P(('dp', 'tp', 'cp'), None)
    gain_spec = P(None, None)
    q_spec = P(None, None, 'tp', None)
    col_spec = P(None, None, 'tp')
    o_spec = P(None, 'tp', None, None)
    down_spec = P(None, 'tp', None)

    def body(tokens, norm_attn, norm_mlp, w_q, w_k, w_v, w_o, w_gate, w_up, w_down):
        wq = jnp.transpose(w_q, (0, 2, 3, 1)).reshape(LAYERS, 1024, D)
        wo = w_o.reshape(LAYERS, 1024, D)
        hbm = pl.BlockSpec(memory_space=pl.ANY)
        vmem = pl.BlockSpec(memory_space=pltpu.VMEM)
        dma = pltpu.SemaphoreType.DMA
        return pl.pallas_call(
            kernel,
            out_shape=jax.ShapeDtypeStruct((ROWS, D), BF16),
            in_specs=[hbm, vmem, vmem] + [hbm] * 8,
            out_specs=hbm,
            scratch_shapes=[
                pltpu.VMEM((NCH, ROWS, CH), BF16),
                pltpu.VMEM((NCH, ROWS, CH), BF16),
                pltpu.VMEM((ROWS, D), BF16),
                pltpu.VMEM((2, 2, 4, 4 * SEG, 128), BF16),
                pltpu.VMEM((2, ROWS, 1024), BF16),
                pltpu.VMEM((2, ROWS, 1024), BF16),
                pltpu.VMEM((LAYERS, 1024, 512), BF16),
                pltpu.VMEM((2, ROWS, FF), BF16),
                pltpu.VMEM((NCH, ROWS, CH), F32),
                pltpu.VMEM((NCH, ROWS, CH), F32),
                pltpu.VMEM((1024, D), BF16),
                pltpu.VMEM((1024, D), BF16),
                pltpu.VMEM((D, 256), BF16),
                pltpu.VMEM((D, 256), BF16),
                pltpu.VMEM((NGC, D, GCH), BF16),
                pltpu.VMEM((NGC, D, GCH), BF16),
                pltpu.VMEM((RING, FF, CH), BF16),
                pltpu.VMEM((2, ROWS, 128), F32),
                pltpu.VMEM((2, ROWS, 128), F32),
                pltpu.VMEM((2, ROWS, 128), F32),
                dma((NCH,)), dma((NCH,)), dma((2,)), dma((2,)), dma((2, NGC)), dma((RING,)), dma((2, 2)),
                dma((NCH,)), dma((NCH,)), dma((NCH,)), dma((NCH,)), dma((2, NCH)), dma((2, NCH)),
                dma((LAYERS, 3, 2, 2)), dma((LAYERS, 3, 2, 2)), dma((2,)), dma((2,)),
                dma((PIECES,)), dma((PIECES,)), dma((3, PIECES)), dma((3, PIECES)),
            ],
            compiler_params=pltpu.CompilerParams(
                collective_id=0, has_side_effects=True, vmem_limit_bytes=67_000_000),
            name='decoder',
        )(tokens, norm_attn, norm_mlp, jnp.asarray(turn_table()),
          wq, w_k, w_v, wo, w_gate, w_up, w_down)

    return jax.shard_map(
        body,
        mesh=mesh,
        in_specs=(row_spec, gain_spec, gain_spec, q_spec, col_spec, col_spec, o_spec, col_spec, col_spec, down_spec),
        out_specs=row_spec,
        check_vma=False,
    )
```

```python
import math

import jax
import jax.numpy as jnp
import numpy as np
from jax import lax
from jax.experimental import pallas as pl
from jax.experimental.pallas import tpu as pltpu
from jax.sharding import PartitionSpec as P

MESH = pl.DeviceIdType.MESH
F32 = jnp.float32
BF16 = jnp.bfloat16
ROWS, SEG, D, HEAD, FF = 128, 64, 2048, 64, 4096
CH, NCH = 256, 8
GCH, NGC = 512, 8
RING = 4
PIECES, PIECE = 16, 16
FIRST, MIDDLE, LATE = range(0, 6), range(6, 10), range(10, 16)
LAYERS = 2
EXP2_SCALE = math.log2(math.e) / math.sqrt(HEAD)


def kernel(tokens, gain_attn, gain_mlp, table, wq, wk, wv, wo, wg, wu, wd, out,
           x_own, x_par, a_ref, qh, o_ref, o_x, kv, act, sbuf, rbuf, slot, wo_x, wk_v, wv_v, wg_v, wu_v, wd_v,
           turns, cos_ref, sin_ref,
           tok_sem, out_sem, slot_sem, kvw_sem, gu_sem, wd_sem, turn_sem, xs_sem, xr_sem, ps_sem, pr_sem, ds_sem, dr_sem,
           ks_sem, kr_sem, os_sem, or_sem, ws_sem, wr_sem, fs_sem, fr_sem):
    t = lax.axis_index('tp')
    c = lax.axis_index('cp')
    other = {'tp': 1 - t}
    beside, across, corner = c + 1 - 2 * lax.rem(c, 2), lax.rem(c + 2, 4), 3 - c
    peers = (beside, across, corner)

    def load_slot(src):
        return [pltpu.make_async_copy(src.at[pl.ds(i * 512, 512)], slot.at[pl.ds(i * 512, 512)], slot_sem.at[i]) for i in range(2)]

    def load_kvw(l):
        return [pltpu.make_async_copy(wk.at[l], wk_v, kvw_sem.at[0]), pltpu.make_async_copy(wv.at[l], wv_v, kvw_sem.at[1])]

    def load_gu(l, j):
        cols = pl.ds(pl.multiple_of(j * GCH, GCH), GCH)
        return [pltpu.make_async_copy(wg.at[l, :, cols], wg_v.at[j], gu_sem.at[0, j]),
                pltpu.make_async_copy(wu.at[l, :, cols], wu_v.at[j], gu_sem.at[1, j])]

    def load_wd(l, j):
        cols = pl.ds(pl.multiple_of(j * CH, CH), CH)
        s = lax.rem(j, RING)
        return pltpu.make_async_copy(wd.at[l, :, cols], wd_v.at[s], wd_sem.at[s])

    def start(copies):
        for copy in copies:
            copy.start()

    def wait(copies):
        for copy in copies:
            copy.wait()

    def send_x(src, j):
        return pltpu.make_async_remote_copy(src, x_par.at[j], xs_sem.at[j], xr_sem.at[j], other, MESH)

    def send_part(j):
        return pltpu.make_async_remote_copy(sbuf.at[j], rbuf.at[j], ps_sem.at[j], pr_sem.at[j], other, MESH)

    def segments(g, ti, ci):
        k = (ti if g == 0 else 1 - ti) * 4 + ci
        return k, 15 - k

    def send_half(i, j):
        place = (j, pl.ds(i * SEG, SEG))
        return pltpu.make_async_remote_copy(sbuf.at[place], rbuf.at[place], ds_sem.at[i, j], dr_sem.at[i, j], other, MESH)

    def send_o(g):
        return pltpu.make_async_remote_copy(o_ref.at[g], o_x.at[1 - g], os_sem.at[g], or_sem.at[1 - g], other, MESH)

    def recv_o(g):
        return pltpu.make_async_remote_copy(o_ref.at[g], o_x.at[g], os_sem.at[g], or_sem.at[g], other, MESH)

    def send_kv(l, kind, g, i, owner, to):
        rows = pl.ds(pl.multiple_of(segments(g, t, owner)[i] * SEG, SEG), SEG)
        place = kv.at[l, rows, :]
        return pltpu.make_async_remote_copy(place, place, ks_sem.at[l, kind, g, i], kr_sem.at[l, kind, g, i], {'cp': to}, MESH)

    def piece(owner, p):
        return pl.ds(pl.multiple_of(owner * (PIECES * PIECE) + p * PIECE, PIECE), PIECE)

    def send_wo(p):
        return pltpu.make_async_remote_copy(wo.at[1, piece(c, p)], wo_x.at[piece(c, p)], ws_sem.at[p], wr_sem.at[p], other, MESH)

    def spread_wo(kind, p, owner, to):
        place = wo_x.at[piece(owner, p)]
        return pltpu.make_async_remote_copy(place, place, fs_sem.at[kind, p], fr_sem.at[kind, p], {'cp': to}, MESH)

    def pass_wo(pieces):
        for p in pieces:
            send_wo(p).wait_recv()
            spread_wo(1, p, c, across).start()
            spread_wo(0, p, c, beside).start()

    def relay_wo(pieces):
        for p in pieces:
            spread_wo(1, p, across, across).wait_recv()
            spread_wo(2, p, across, beside).start()

    tok = [pltpu.make_async_copy(tokens.at[:, pl.ds(j * CH, CH)], x_own.at[j], tok_sem.at[j]) for j in range(NCH)]
    start(tok)
    turn = [pltpu.make_async_copy(table.at[pl.ds(pl.multiple_of(segments(g, t, c)[i] * SEG, SEG), SEG)],
                                  turns.at[g, pl.ds(i * SEG, SEG)], turn_sem.at[g, i]) for g in range(2) for i in range(2)]
    start(turn)
    start(load_kvw(0))
    start(load_slot(wq.at[0]))

    barrier = pltpu.get_barrier_semaphore()
    pl.semaphore_signal(barrier, inc=1, device_id=other, device_id_type=MESH)
    for to in peers:
        pl.semaphore_signal(barrier, inc=1, device_id={'cp': to}, device_id_type=MESH)
    pl.semaphore_wait(barrier, 4)
    for j in range(NCH):
        send_x(tokens.at[:, pl.ds(j * CH, CH)], j).start()
    for p in FIRST:
        send_wo(p).start()
    for j in range(NGC):
        start(load_gu(0, j))
    for j in range(RING):
        load_wd(0, j).start()

    lane = lax.broadcasted_iota(jnp.int32, (ROWS, 128), 1)
    first_half = (lane % HEAD) < HEAD // 2
    low = lane < HEAD
    low_seg = lax.broadcasted_iota(jnp.int32, (SEG, 128), 1) < HEAD
    diff = (lax.broadcasted_iota(jnp.int32, (4 * SEG, 512), 1)
            - lax.broadcasted_iota(jnp.int32, (4 * SEG, 512), 0) % SEG)

    wait(turn)
    for g in range(2):
        near, far = turns[g], pltpu.roll(turns[g], HEAD, 1)
        cos_ref[g] = jnp.where(low, near, far)
        sin_ref[g] = jnp.where(low, far, near)

    def norm(x_ref, gain_ref, l):
        total = jnp.zeros((ROWS, 1), F32)
        for j in range(NCH):
            x = x_ref[j].astype(F32)
            total = total + jnp.sum(x * x, axis=-1, keepdims=True)
        inv = lax.rsqrt(total * (1.0 / D) + 1e-5)
        for j in range(NCH):
            cols = pl.ds(j * CH, CH)
            a_ref[:, cols] = (x_ref[j].astype(F32) * inv * gain_ref[l:l + 1, cols].astype(F32)).astype(BF16)

    def rope(v, g):
        swapped = jnp.where(first_half, pltpu.roll(v, 128 - HEAD // 2, 1), pltpu.roll(v, HEAD // 2, 1))
        return v * cos_ref[g] + swapped * sin_ref[g]

    def qkv(l, g):
        k_new = jnp.dot(a_ref[...], wk_v[...], preferred_element_type=F32)
        v_new = jnp.dot(a_ref[...], wv_v[...], preferred_element_type=F32).astype(BF16)
        k_new = jnp.concatenate([rope(k_new[:, :128], g), rope(k_new[:, 128:], g)], axis=1).astype(BF16)
        for i in range(2):
            rows = pl.ds(pl.multiple_of(segments(g, t, c)[i] * SEG, SEG), SEG)
            kv[l, rows, 0:256] = k_new[i * SEG:(i + 1) * SEG]
            kv[l, rows, 256:512] = v_new[i * SEG:(i + 1) * SEG]
        for i in range(2):
            for kind in ((1, 2, 0) if g == 0 else (1, 0)):
                send_kv(l, kind, g, i, c, peers[kind]).start()
        for h in range(4):
            q = lax.dot_general(a_ref[...], slot[h * 256:(h + 1) * 256, :], (((1,), (1,)), ((), ())), preferred_element_type=F32)
            for pair in range(2):
                both = rope(q[:, pair * 128:(pair + 1) * 128], g)
                turned = pltpu.roll(both, HEAD, 1)
                for odd in range(2):
                    value = both if odd == h % 2 else turned
                    value = jnp.where(low if h % 2 == 0 else ~low, value, 0.0).astype(BF16)
                    n = pair * 2 + odd
                    for i in range(2):
                        qh[g, i, h, n * SEG:(n + 1) * SEG, :] = value[i * SEG:(i + 1) * SEG]

    def attention(l, g, parts=(0, 1)):
        for i in parts:
            seg = segments(g, t, c)[i]
            free = 512 * i
            visible = diff <= seg * SEG - free
            for parity in range(2):
                def pair_step(p, carry, i=i, free=free, visible=visible, parity=parity):
                    h = 2 * p + parity
                    k_cols = pl.ds(pl.multiple_of(p * 128, 128), 128)
                    v_cols = pl.ds(pl.multiple_of(256 + p * 128, 128), 128)
                    q = qh[g, i, h]
                    nt = (((1,), (1,)), ((), ()))
                    s_end = lax.dot_general(q, kv[l, pl.ds(free, 512), k_cols], nt, preferred_element_type=F32)
                    s_end = jnp.where(visible, s_end, -jnp.inf)
                    top = jnp.max(s_end, axis=-1, keepdims=True)
                    if free:
                        s_free = lax.dot_general(q, kv[l, pl.ds(0, free), k_cols], nt, preferred_element_type=F32)
                        top = jnp.maximum(top, jnp.max(s_free, axis=-1, keepdims=True))
                    e_end = jnp.exp2((s_end - top) * EXP2_SCALE)
                    total = jnp.sum(e_end, axis=-1, keepdims=True)
                    mixed = jnp.dot(e_end.astype(BF16), kv[l, pl.ds(free, 512), v_cols], preferred_element_type=F32)
                    if free:
                        e_free = jnp.exp2((s_free - top) * EXP2_SCALE)
                        total = total + jnp.sum(e_free, axis=-1, keepdims=True)
                        mixed = mixed + jnp.dot(e_free.astype(BF16), kv[l, pl.ds(0, free), v_cols], preferred_element_type=F32)
                    mixed = mixed / total
                    for pair in range(2):
                        sides = []
                        for odd in range(2):
                            n = pair * 2 + odd
                            value = mixed[n * SEG:(n + 1) * SEG]
                            sides.append(value if odd == parity else pltpu.roll(value, HEAD, 1))
                        cols = pl.ds(pl.multiple_of(h * 256 + pair * 128, 128), 128)
                        o_ref[g, i * SEG:(i + 1) * SEG, cols] = jnp.where(low_seg, sides[0], sides[1]).astype(BF16)
                    return carry
                lax.fori_loop(0, 2, pair_step, 0)

    def slot_chunk(lhs, j):
        return jnp.dot(lhs, slot[:, pl.ds(pl.multiple_of(j * CH, CH), CH)], preferred_element_type=F32)

    def reduce_chunk(own, j):
        return (x_own[j].astype(F32) + (own + rbuf[j])).astype(BF16)

    for l in range(LAYERS):
        last = l == LAYERS - 1
        if l == 0:
            wait(tok)
        norm(x_own, gain_attn, l)
        wait(load_kvw(l))
        wait(load_slot(wq.at[l]))
        qkv(l, 0)
        for j in range(NCH):
            send_x(x_own.at[j], j).wait_recv()
        norm(x_par, gain_attn, l)
        qkv(l, 1)
        start(load_slot(wo.at[l]))
        if not last:
            start(load_kvw(l + 1))
        for i in range(2):
            send_kv(l, 1, 1, i, across, across).wait_recv()
            send_kv(l, 2, 1, i, across, beside).start()

        def wait_kv(i, l=l):
            for kind, g in ((0, 0), (1, 0), (2, 0), (0, 1), (2, 1)):
                send_kv(l, kind, g, i, peers[kind], peers[kind]).wait_recv()

        wait_kv(0)
        if not last:
            wait(load_slot(wo.at[l]))
            for i in range(2):
                if i == 1:
                    wait_kv(1)
                attention(l, 1, (i,))

                def o_send(j, carry, i=i):
                    rows = pl.ds(i * SEG, SEG)
                    sbuf[j, rows] = slot_chunk(o_ref[1, rows], j)
                    send_half(i, j).start()
                    return carry
                lax.fori_loop(0, NCH, o_send, 0)
            pass_wo(FIRST)
            attention(l, 0)

            def o_reduce(j, carry):
                own = slot_chunk(o_ref[0], j)
                send_half(0, j).wait_recv()
                send_half(1, j).wait_recv()
                new = reduce_chunk(own, j)
                send_x(x_own.at[j], j).wait_send()
                x_own[j] = new
                send_x(x_own.at[j], j).start()
                return carry
            lax.fori_loop(0, NCH, o_reduce, 0)
            for p in MIDDLE:
                send_wo(p).start()
            relay_wo(FIRST)
            start(load_slot(wq.at[l + 1]))
        else:
            pass_wo(LATE[:2])
            attention(l, 0, (0,))
            wait_kv(1)
            attention(l, 0, (1,))
            send_o(0).start()
            pass_wo(LATE[2:5])
            relay_wo(LATE[:2])
            attention(l, 1, (0,))
            pass_wo(LATE[5:])
            attention(l, 1, (1,))
            send_o(1).start()
            relay_wo(LATE[2:5])
            wait(load_slot(wo.at[l]))

            def o_near(j, carry):
                send_part(j).wait_send()
                sbuf[j] = slot_chunk(o_ref[1], j)
                return carry
            lax.fori_loop(0, NCH, o_near, 0)
            relay_wo(LATE[5:])
            for p in range(PIECES):
                spread_wo(0, p, beside, beside).wait_recv()
                spread_wo(2, p, corner, beside).wait_recv()

        def gate_up(g, l=l, last=last):
            def step(j, carry):
                if g == (1 if last else 0):
                    wait(load_gu(l, j))
                gate = jnp.dot(a_ref[...], wg_v[j], preferred_element_type=F32)
                up = jnp.dot(a_ref[...], wu_v[j], preferred_element_type=F32)
                act[g, :, pl.ds(pl.multiple_of(j * GCH, GCH), GCH)] = (gate * jax.nn.sigmoid(gate) * up).astype(BF16)
                if g == 1 and not last:
                    start(load_gu(l + 1, j))
                return carry
            lax.fori_loop(0, NGC, step, 0)

        def far_chunk(g, j):
            return jnp.dot(o_x[g], wo_x[:, pl.ds(pl.multiple_of(j * CH, CH), CH)], preferred_element_type=F32)

        if not last:
            norm(x_own, gain_mlp, l)
            gate_up(0)
            for j in range(NCH):
                send_x(x_own.at[j], j).wait_recv()
            norm(x_par, gain_mlp, l)
            gate_up(1)
        else:
            recv_o(1).wait_recv()

            def o_far(j, carry):
                x_par[j] = (x_par[j].astype(F32) + (sbuf[j] + far_chunk(1, j))).astype(BF16)
                return carry
            lax.fori_loop(0, NCH, o_far, 0)
            norm(x_par, gain_mlp, l)
            gate_up(1)

        def down_chunk(g, j, l=l):
            load_wd(l, j).wait()
            return jnp.dot(act[g], wd_v[lax.rem(j, RING)], preferred_element_type=F32)

        def down_send(j, carry, l=l, last=last):
            part = down_chunk(1, j)
            load_wd(l, lax.rem(j + RING, NCH)).start()
            if not last:
                send_half(0, j).wait_send()
                send_half(1, j).wait_send()
            sbuf[j] = part
            send_part(j).start()
            return carry
        lax.fori_loop(0, NCH, down_send, 0)
        if not last:
            pass_wo(MIDDLE)
        else:
            recv_o(0).wait_recv()

            def o_own(j, carry):
                new = (x_own[j].astype(F32) + (slot_chunk(o_ref[0], j) + far_chunk(0, j))).astype(BF16)
                send_x(x_own.at[j], j).wait_send()
                x_own[j] = new
                return carry
            lax.fori_loop(0, NCH, o_own, 0)
            norm(x_own, gain_mlp, l)
            gate_up(0)

        def down_reduce(j, carry, l=l, last=last):
            own = down_chunk(0, j)
            if last:
                @pl.when(j < NCH - RING)
                def _():
                    load_wd(l, j + RING).start()
            else:
                @pl.when(j < NCH - RING)
                def _():
                    load_wd(l, j + RING).start()

                @pl.when(j >= NCH - RING)
                def _():
                    load_wd(l + 1, j + RING - NCH).start()
            send_part(j).wait_recv()
            new = reduce_chunk(own, j)
            if not last:
                send_x(x_own.at[j], j).wait_send()
            x_own[j] = new
            cols = pl.ds(pl.multiple_of(j * CH, CH), CH)
            if last:
                pltpu.make_async_copy(x_own.at[j], out.at[:, cols], out_sem.at[j]).start()
            else:
                send_x(x_own.at[j], j).start()
            return carry
        lax.fori_loop(0, NCH, down_reduce, 0)
        if not last:
            for p in LATE:
                send_wo(p).start()
            relay_wo(MIDDLE)

    for j in range(NCH):
        send_part(j).wait_send()
        pltpu.make_async_copy(x_own.at[j], out.at[:, pl.ds(j * CH, CH)], out_sem.at[j]).wait()
    for l in range(LAYERS):
        for g in range(2):
            for i in range(2):
                for kind in range(3):
                    send_kv(l, kind, g, i, c, beside).wait_send()
    for g in range(2):
        send_o(g).wait_send()
    for p in range(PIECES):
        send_wo(p).wait_send()
        for kind in range(3):
            spread_wo(kind, p, c, beside).wait_send()


def turn_table():
    inv_freq = np.float32(500000.0) ** (-(np.arange(HEAD // 2, dtype=np.float32) * np.float32(2.0) / np.float32(HEAD)))
    angles = np.arange(16 * SEG, dtype=np.float32)[:, None] * inv_freq.astype(np.float32)[None, :]
    cos, sin = np.cos(angles), np.sin(angles)
    return np.concatenate([cos, cos, -sin, sin], axis=1).astype(np.float32)


def solution(mesh):
    tp_size = mesh.shape['tp']
    cp_size = mesh.shape['cp']
    row_spec = P(('dp', 'tp', 'cp'), None)
    gain_spec = P(None, None)
    q_spec = P(None, None, 'tp', None)
    col_spec = P(None, None, 'tp')
    o_spec = P(None, 'tp', None, None)
    down_spec = P(None, 'tp', None)

    def body(tokens, norm_attn, norm_mlp, w_q, w_k, w_v, w_o, w_gate, w_up, w_down):
        wq = jnp.transpose(w_q, (0, 2, 3, 1)).reshape(LAYERS, 1024, D)
        wo = w_o.reshape(LAYERS, 1024, D)
        hbm = pl.BlockSpec(memory_space=pl.ANY)
        vmem = pl.BlockSpec(memory_space=pltpu.VMEM)
        dma = pltpu.SemaphoreType.DMA
        return pl.pallas_call(
            kernel,
            out_shape=jax.ShapeDtypeStruct((ROWS, D), BF16),
            in_specs=[hbm, vmem, vmem] + [hbm] * 8,
            out_specs=hbm,
            scratch_shapes=[
                pltpu.VMEM((NCH, ROWS, CH), BF16),
                pltpu.VMEM((NCH, ROWS, CH), BF16),
                pltpu.VMEM((ROWS, D), BF16),
                pltpu.VMEM((2, 2, 4, 4 * SEG, 128), BF16),
                pltpu.VMEM((2, ROWS, 1024), BF16),
                pltpu.VMEM((2, ROWS, 1024), BF16),
                pltpu.VMEM((LAYERS, 1024, 512), BF16),
                pltpu.VMEM((2, ROWS, FF), BF16),
                pltpu.VMEM((NCH, ROWS, CH), F32),
                pltpu.VMEM((NCH, ROWS, CH), F32),
                pltpu.VMEM((1024, D), BF16),
                pltpu.VMEM((1024, D), BF16),
                pltpu.VMEM((D, 256), BF16),
                pltpu.VMEM((D, 256), BF16),
                pltpu.VMEM((NGC, D, GCH), BF16),
                pltpu.VMEM((NGC, D, GCH), BF16),
                pltpu.VMEM((RING, FF, CH), BF16),
                pltpu.VMEM((2, ROWS, 128), F32),
                pltpu.VMEM((2, ROWS, 128), F32),
                pltpu.VMEM((2, ROWS, 128), F32),
                dma((NCH,)), dma((NCH,)), dma((2,)), dma((2,)), dma((2, NGC)), dma((RING,)), dma((2, 2)),
                dma((NCH,)), dma((NCH,)), dma((NCH,)), dma((NCH,)), dma((2, NCH)), dma((2, NCH)),
                dma((LAYERS, 3, 2, 2)), dma((LAYERS, 3, 2, 2)), dma((2,)), dma((2,)),
                dma((PIECES,)), dma((PIECES,)), dma((3, PIECES)), dma((3, PIECES)),
            ],
            compiler_params=pltpu.CompilerParams(
                collective_id=0, has_side_effects=True, vmem_limit_bytes=67_000_000),
            name='decoder',
        )(tokens, norm_attn, norm_mlp, jnp.asarray(turn_table()),
          wq, w_k, w_v, wo, w_gate, w_up, w_down)

    return jax.shard_map(
        body,
        mesh=mesh,
        in_specs=(row_spec, gain_spec, gain_spec, q_spec, col_spec, col_spec, o_spec, col_spec, col_spec, down_spec),
        out_specs=row_spec,
        check_vma=False,
    )
```

```python
import functools
import math

import jax
import jax.numpy as jnp
import numpy as np
from jax import lax
from jax.experimental import pallas as pl
from jax.experimental.pallas import tpu as pltpu
from jax.sharding import PartitionSpec as P

MESH = pl.DeviceIdType.MESH
F32 = jnp.float32
BF16 = jnp.bfloat16
ROWS, SEG, D, HEAD, FF = 128, 64, 2048, 64, 4096
CH, NCH = 256, 8
GCH, NGC = 512, 8
RING = 4
PIECES, PIECE = 16, 16
FIRST, MIDDLE, LATE = range(0, 7), range(7, 12), range(12, 16)
LAYERS = 2
EXP2_SCALE = math.log2(math.e) / math.sqrt(HEAD)


def kernel(tokens, gain_attn, gain_mlp, table, wq, wk, wv, wo, wg, wu, wd, out,
           x_own, x_par, a_ref, qh, o_ref, o_x, kv, act, sbuf, rbuf, slot, wo_x, wk_v, wv_v, wg_v, wu_v, wd_v,
           turns, cos_ref, sin_ref,
           tok_sem, out_sem, slot_sem, kvw_sem, gu_sem, wd_sem, turn_sem, xs_sem, xr_sem, ps_sem, pr_sem, ds_sem, dr_sem,
           ks_sem, kr_sem, os_sem, or_sem, ws_sem, wr_sem, fs_sem, fr_sem):
    t = lax.axis_index('tp')
    c = lax.axis_index('cp')
    other = {'tp': 1 - t}
    beside, across, corner = c + 1 - 2 * lax.rem(c, 2), lax.rem(c + 2, 4), 3 - c
    peers = (beside, across, corner)

    def load_slot(src):
        return [pltpu.make_async_copy(src.at[pl.ds(i * 512, 512)], slot.at[pl.ds(i * 512, 512)], slot_sem.at[i]) for i in range(2)]

    def load_kvw(l):
        return [pltpu.make_async_copy(wk.at[l], wk_v, kvw_sem.at[0]), pltpu.make_async_copy(wv.at[l], wv_v, kvw_sem.at[1])]

    def load_gu(l, j):
        cols = pl.ds(pl.multiple_of(j * GCH, GCH), GCH)
        return [pltpu.make_async_copy(wg.at[l, :, cols], wg_v.at[j], gu_sem.at[0, j]),
                pltpu.make_async_copy(wu.at[l, :, cols], wu_v.at[j], gu_sem.at[1, j])]

    def load_wd(l, j):
        cols = pl.ds(pl.multiple_of(j * CH, CH), CH)
        s = lax.rem(j, RING)
        return pltpu.make_async_copy(wd.at[l, :, cols], wd_v.at[s], wd_sem.at[s])

    def start(copies):
        for copy in copies:
            copy.start()

    def wait(copies):
        for copy in copies:
            copy.wait()

    def send_x(src, j):
        return pltpu.make_async_remote_copy(src, x_par.at[j], xs_sem.at[j], xr_sem.at[j], other, MESH)

    def send_part(j):
        return pltpu.make_async_remote_copy(sbuf.at[j], rbuf.at[j], ps_sem.at[j], pr_sem.at[j], other, MESH)

    def segments(g, ti, ci):
        k = (ti if g == 0 else 1 - ti) * 4 + ci
        return k, 15 - k

    def send_half(i, j):
        place = (j, pl.ds(i * SEG, SEG))
        return pltpu.make_async_remote_copy(sbuf.at[place], rbuf.at[place], ds_sem.at[i, j], dr_sem.at[i, j], other, MESH)

    def send_o(g, i):
        rows = pl.ds(i * SEG, SEG)
        return pltpu.make_async_remote_copy(o_ref.at[g, rows], o_x.at[1 - g, rows], os_sem.at[g, i], or_sem.at[1 - g, i], other, MESH)

    def recv_o(g, i):
        rows = pl.ds(i * SEG, SEG)
        return pltpu.make_async_remote_copy(o_ref.at[g, rows], o_x.at[g, rows], os_sem.at[g, i], or_sem.at[g, i], other, MESH)

    def send_kv(l, kind, g, i, owner, to):
        rows = pl.ds(pl.multiple_of(segments(g, t, owner)[i] * SEG, SEG), SEG)
        place = kv.at[l, rows, :]
        return pltpu.make_async_remote_copy(place, place, ks_sem.at[l, kind, g, i], kr_sem.at[l, kind, g, i], {'cp': to}, MESH)

    def piece(owner, p):
        return pl.ds(pl.multiple_of(owner * (PIECES * PIECE) + p * PIECE, PIECE), PIECE)

    def send_wo(p):
        return pltpu.make_async_remote_copy(wo.at[1, piece(c, p)], wo_x.at[piece(c, p)], ws_sem.at[p], wr_sem.at[p], other, MESH)

    def spread_wo(kind, p, owner, to):
        place = wo_x.at[piece(owner, p)]
        return pltpu.make_async_remote_copy(place, place, fs_sem.at[kind, p], fr_sem.at[kind, p], {'cp': to}, MESH)

    def pass_wo(pieces):
        for p in pieces:
            send_wo(p).wait_recv()
            spread_wo(1, p, c, across).start()
            spread_wo(0, p, c, beside).start()

    def relay_wo(pieces):
        for p in pieces:
            spread_wo(1, p, across, across).wait_recv()
            spread_wo(2, p, across, beside).start()

    tok = [pltpu.make_async_copy(tokens.at[:, pl.ds(j * CH, CH)], x_own.at[j], tok_sem.at[j]) for j in range(NCH)]
    start(tok)
    turn = [pltpu.make_async_copy(table.at[pl.ds(pl.multiple_of(segments(g, t, c)[i] * SEG, SEG), SEG)],
                                  turns.at[g, pl.ds(i * SEG, SEG)], turn_sem.at[g, i]) for g in range(2) for i in range(2)]
    start(turn)
    start(load_kvw(0))
    start(load_slot(wq.at[0]))

    barrier = pltpu.get_barrier_semaphore()
    pl.semaphore_signal(barrier, inc=1, device_id=other, device_id_type=MESH)
    for to in peers:
        pl.semaphore_signal(barrier, inc=1, device_id={'cp': to}, device_id_type=MESH)
    pl.semaphore_wait(barrier, 4)
    for j in range(NCH):
        send_x(tokens.at[:, pl.ds(j * CH, CH)], j).start()
    for p in FIRST:
        send_wo(p).start()
    for j in range(RING):
        load_wd(0, j).start()

    lane = lax.broadcasted_iota(jnp.int32, (ROWS, 128), 1)
    first_half = (lane % HEAD) < HEAD // 2
    low = lane < HEAD
    low_seg = lax.broadcasted_iota(jnp.int32, (SEG, 128), 1) < HEAD
    diff = (lax.broadcasted_iota(jnp.int32, (4 * SEG, 512), 1)
            - lax.broadcasted_iota(jnp.int32, (4 * SEG, 512), 0) % SEG)

    wait(turn)
    for g in range(2):
        near, far = turns[g], pltpu.roll(turns[g], HEAD, 1)
        cos_ref[g] = jnp.where(low, near, far)
        sin_ref[g] = jnp.where(low, far, near)

    def norm(x_ref, gain_ref, l):
        total = jnp.zeros((ROWS, 1), F32)
        for j in range(NCH):
            x = x_ref[j].astype(F32)
            total = total + jnp.sum(x * x, axis=-1, keepdims=True)
        inv = lax.rsqrt(total * (1.0 / D) + 1e-5)
        for j in range(NCH):
            cols = pl.ds(j * CH, CH)
            a_ref[:, cols] = (x_ref[j].astype(F32) * inv * gain_ref[l:l + 1, cols].astype(F32)).astype(BF16)

    def rope(v, g):
        swapped = jnp.where(first_half, pltpu.roll(v, 128 - HEAD // 2, 1), pltpu.roll(v, HEAD // 2, 1))
        return v * cos_ref[g] + swapped * sin_ref[g]

    def qkv(l, g):
        k_new = jnp.dot(a_ref[...], wk_v[...], preferred_element_type=F32)
        v_new = jnp.dot(a_ref[...], wv_v[...], preferred_element_type=F32).astype(BF16)
        k_new = jnp.concatenate([rope(k_new[:, :128], g), rope(k_new[:, 128:], g)], axis=1).astype(BF16)
        for i in range(2):
            rows = pl.ds(pl.multiple_of(segments(g, t, c)[i] * SEG, SEG), SEG)
            kv[l, rows, 0:256] = k_new[i * SEG:(i + 1) * SEG]
            kv[l, rows, 256:512] = v_new[i * SEG:(i + 1) * SEG]
        for i in range(2):
            for kind in ((1, 2, 0) if g == 0 else (1, 0)):
                send_kv(l, kind, g, i, c, peers[kind]).start()
        for h in range(4):
            q = lax.dot_general(a_ref[...], slot[h * 256:(h + 1) * 256, :], (((1,), (1,)), ((), ())), preferred_element_type=F32)
            for pair in range(2):
                both = rope(q[:, pair * 128:(pair + 1) * 128], g)
                turned = pltpu.roll(both, HEAD, 1)
                for odd in range(2):
                    value = both if odd == h % 2 else turned
                    value = jnp.where(low if h % 2 == 0 else ~low, value, 0.0).astype(BF16)
                    n = pair * 2 + odd
                    for i in range(2):
                        qh[g, i, h, n * SEG:(n + 1) * SEG, :] = value[i * SEG:(i + 1) * SEG]

    def attention(l, g, parts=(0, 1)):
        for i in parts:
            seg = segments(g, t, c)[i]
            free = 512 * i
            visible = diff <= seg * SEG - free

            def pair_step(p, carry, i=i, free=free, visible=visible):
                k_cols = pl.ds(pl.multiple_of(p * 128, 128), 128)
                v_cols = pl.ds(pl.multiple_of(256 + p * 128, 128), 128)
                nt = (((1,), (1,)), ((), ()))
                spans = ((free, 512), (0, 512)) if free else ((free, 512),)
                scores, tops, totals, outs = {}, {}, {}, {}
                for parity in range(2):
                    q = qh[g, i, 2 * p + parity]
                    for n, (lo, size) in enumerate(spans):
                        s = lax.dot_general(q, kv[l, pl.ds(lo, size), k_cols], nt, preferred_element_type=F32)
                        scores[parity, n] = jnp.where(visible, s, -jnp.inf) if n == 0 else s
                for parity in range(2):
                    tops[parity] = functools.reduce(jnp.maximum, [jnp.max(scores[parity, n], axis=-1, keepdims=True) for n in range(len(spans))])
                    total, mixed = 0.0, 0.0
                    for n, (lo, size) in enumerate(spans):
                        e = jnp.exp2((scores[parity, n] - tops[parity]) * EXP2_SCALE)
                        total = total + jnp.sum(e, axis=-1, keepdims=True)
                        mixed = mixed + jnp.dot(e.astype(BF16), kv[l, pl.ds(lo, size), v_cols], preferred_element_type=F32)
                    mixed = mixed / total
                    for pair in range(2):
                        sides = []
                        for odd in range(2):
                            n = pair * 2 + odd
                            value = mixed[n * SEG:(n + 1) * SEG]
                            sides.append(value if odd == parity else pltpu.roll(value, HEAD, 1))
                        cols = pl.ds(pl.multiple_of((2 * p + parity) * 256 + pair * 128, 128), 128)
                        o_ref[g, i * SEG:(i + 1) * SEG, cols] = jnp.where(low_seg, sides[0], sides[1]).astype(BF16)
                return carry
            lax.fori_loop(0, 2, pair_step, 0)

    def slot_chunk(lhs, j):
        return jnp.dot(lhs, slot[:, pl.ds(pl.multiple_of(j * CH, CH), CH)], preferred_element_type=F32)

    def reduce_chunk(own, j):
        return (x_own[j].astype(F32) + (own + rbuf[j])).astype(BF16)

    for l in range(LAYERS):
        last = l == LAYERS - 1
        if l == 0:
            wait(tok)
        norm(x_own, gain_attn, l)
        wait(load_kvw(l))
        wait(load_slot(wq.at[l]))
        qkv(l, 0)
        for j in range(NCH):
            send_x(x_own.at[j], j).wait_recv()
        norm(x_par, gain_attn, l)
        qkv(l, 1)
        start(load_slot(wo.at[l]))
        if not last:
            start(load_kvw(l + 1))
        if last:
            pass_wo(LATE[:1])
        for i in range(2):
            send_kv(l, 1, 1, i, across, across).wait_recv()
            send_kv(l, 2, 1, i, across, beside).start()
            if last and i == 0:
                pass_wo(LATE[1:3])

        def wait_kv(i, l=l):
            for kind, g in ((0, 0), (1, 0), (2, 0), (0, 1), (2, 1)):
                send_kv(l, kind, g, i, peers[kind], peers[kind]).wait_recv()

        wait_kv(0)
        if not last:
            wait(load_slot(wo.at[l]))
            for i in range(2):
                if i == 1:
                    wait_kv(1)
                attention(l, 1, (i,))

                def o_send(j, carry, i=i):
                    rows = pl.ds(i * SEG, SEG)
                    sbuf[j, rows] = slot_chunk(o_ref[1, rows], j)
                    send_half(i, j).start()
                    return carry
                lax.fori_loop(0, NCH, o_send, 0)
            pass_wo(FIRST)
            attention(l, 0)

            def o_reduce(j, carry):
                own = slot_chunk(o_ref[0], j)
                start(load_gu(0, j))
                send_half(0, j).wait_recv()
                send_half(1, j).wait_recv()
                new = reduce_chunk(own, j)
                send_x(x_own.at[j], j).wait_send()
                x_own[j] = new
                send_x(x_own.at[j], j).start()
                return carry
            lax.fori_loop(0, NCH, o_reduce, 0)
            for p in MIDDLE:
                send_wo(p).start()
            relay_wo(FIRST)
            start(load_slot(wq.at[l + 1]))
        else:
            pass_wo(LATE[3:])
            attention(l, 0, (0,))
            send_o(0, 0).start()
            wait_kv(1)
            attention(l, 0, (1,))
            send_o(0, 1).start()
            relay_wo(LATE[:1])
            attention(l, 1, (0,))
            send_o(1, 0).start()
            relay_wo(LATE[1:])
            attention(l, 1, (1,))
            send_o(1, 1).start()
            wait(load_slot(wo.at[l]))

            def o_near(j, carry):
                send_part(j).wait_send()
                sbuf[j] = slot_chunk(o_ref[1], j)
                return carry
            lax.fori_loop(0, NCH, o_near, 0)
            for p in range(PIECES):
                spread_wo(0, p, beside, beside).wait_recv()
                spread_wo(2, p, corner, beside).wait_recv()

        def gate_up(g, l=l, last=last):
            def step(j, carry):
                if g == (1 if last else 0):
                    wait(load_gu(l, j))
                gate = jnp.dot(a_ref[...], wg_v[j], preferred_element_type=F32)
                up = jnp.dot(a_ref[...], wu_v[j], preferred_element_type=F32)
                act[g, :, pl.ds(pl.multiple_of(j * GCH, GCH), GCH)] = (gate * jax.nn.sigmoid(gate) * up).astype(BF16)
                return carry
            lax.fori_loop(0, NGC, step, 0)

        def far_chunk(g, j):
            return jnp.dot(o_x[g], wo_x[:, pl.ds(pl.multiple_of(j * CH, CH), CH)], preferred_element_type=F32)

        if not last:
            norm(x_own, gain_mlp, l)
            gate_up(0)
            for j in range(NCH):
                send_x(x_own.at[j], j).wait_recv()
            norm(x_par, gain_mlp, l)
            gate_up(1)
        else:
            recv_o(1, 0).wait_recv()
            recv_o(1, 1).wait_recv()

            def o_far(j, carry):
                x_par[j] = (x_par[j].astype(F32) + (sbuf[j] + far_chunk(1, j))).astype(BF16)
                return carry
            lax.fori_loop(0, NCH, o_far, 0)
            norm(x_par, gain_mlp, l)
            gate_up(1)

        def down_chunk(g, j, l=l):
            load_wd(l, j).wait()
            return jnp.dot(act[g], wd_v[lax.rem(j, RING)], preferred_element_type=F32)

        def down_send(j, carry, l=l, last=last):
            part = down_chunk(1, j)
            load_wd(l, lax.rem(j + RING, NCH)).start()
            if not last:
                send_half(0, j).wait_send()
                send_half(1, j).wait_send()
            sbuf[j] = part
            send_part(j).start()
            return carry
        lax.fori_loop(0, NCH, down_send, 0)
        if not last:
            pass_wo(MIDDLE)
        else:
            recv_o(0, 0).wait_recv()
            recv_o(0, 1).wait_recv()

            def o_own(j, carry):
                new = (x_own[j].astype(F32) + (slot_chunk(o_ref[0], j) + far_chunk(0, j))).astype(BF16)
                send_x(x_own.at[j], j).wait_send()
                x_own[j] = new
                return carry
            lax.fori_loop(0, NCH, o_own, 0)
            norm(x_own, gain_mlp, l)
            gate_up(0)

        def down_reduce(j, carry, l=l, last=last):
            own = down_chunk(0, j)
            if last:
                @pl.when(j < NCH - RING)
                def _():
                    load_wd(l, j + RING).start()
            else:
                @pl.when(j < NCH - RING)
                def _():
                    load_wd(l, j + RING).start()

                @pl.when(j >= NCH - RING)
                def _():
                    load_wd(l + 1, j + RING - NCH).start()
            if not last:
                start(load_gu(l + 1, j))
            send_part(j).wait_recv()
            new = reduce_chunk(own, j)
            if not last:
                send_x(x_own.at[j], j).wait_send()
            x_own[j] = new
            cols = pl.ds(pl.multiple_of(j * CH, CH), CH)
            if last:
                pltpu.make_async_copy(x_own.at[j], out.at[:, cols], out_sem.at[j]).start()
            else:
                send_x(x_own.at[j], j).start()
            return carry
        lax.fori_loop(0, NCH, down_reduce, 0)
        if not last:
            for p in LATE:
                send_wo(p).start()
            relay_wo(MIDDLE)

    for j in range(NCH):
        send_part(j).wait_send()
        pltpu.make_async_copy(x_own.at[j], out.at[:, pl.ds(j * CH, CH)], out_sem.at[j]).wait()
    for l in range(LAYERS):
        for g in range(2):
            for i in range(2):
                for kind in range(3):
                    send_kv(l, kind, g, i, c, beside).wait_send()
    for g in range(2):
        send_o(g, 0).wait_send()
        send_o(g, 1).wait_send()
    for p in range(PIECES):
        send_wo(p).wait_send()
        for kind in range(3):
            spread_wo(kind, p, c, beside).wait_send()


def turn_table():
    inv_freq = np.float32(500000.0) ** (-(np.arange(HEAD // 2, dtype=np.float32) * np.float32(2.0) / np.float32(HEAD)))
    angles = np.arange(16 * SEG, dtype=np.float32)[:, None] * inv_freq.astype(np.float32)[None, :]
    cos, sin = np.cos(angles), np.sin(angles)
    return np.concatenate([cos, cos, -sin, sin], axis=1).astype(np.float32)


def solution(mesh):
    tp_size = mesh.shape['tp']
    cp_size = mesh.shape['cp']
    row_spec = P(('dp', 'tp', 'cp'), None)
    gain_spec = P(None, None)
    q_spec = P(None, None, 'tp', None)
    col_spec = P(None, None, 'tp')
    o_spec = P(None, 'tp', None, None)
    down_spec = P(None, 'tp', None)

    def body(tokens, norm_attn, norm_mlp, w_q, w_k, w_v, w_o, w_gate, w_up, w_down):
        wq = jnp.transpose(w_q, (0, 2, 3, 1)).reshape(LAYERS, 1024, D)
        wo = w_o.reshape(LAYERS, 1024, D)
        hbm = pl.BlockSpec(memory_space=pl.ANY)
        vmem = pl.BlockSpec(memory_space=pltpu.VMEM)
        dma = pltpu.SemaphoreType.DMA
        return pl.pallas_call(
            kernel,
            out_shape=jax.ShapeDtypeStruct((ROWS, D), BF16),
            in_specs=[hbm, vmem, vmem] + [hbm] * 8,
            out_specs=hbm,
            scratch_shapes=[
                pltpu.VMEM((NCH, ROWS, CH), BF16),
                pltpu.VMEM((NCH, ROWS, CH), BF16),
                pltpu.VMEM((ROWS, D), BF16),
                pltpu.VMEM((2, 2, 4, 4 * SEG, 128), BF16),
                pltpu.VMEM((2, ROWS, 1024), BF16),
                pltpu.VMEM((2, ROWS, 1024), BF16),
                pltpu.VMEM((LAYERS, 1024, 512), BF16),
                pltpu.VMEM((2, ROWS, FF), BF16),
                pltpu.VMEM((NCH, ROWS, CH), F32),
                pltpu.VMEM((NCH, ROWS, CH), F32),
                pltpu.VMEM((1024, D), BF16),
                pltpu.VMEM((1024, D), BF16),
                pltpu.VMEM((D, 256), BF16),
                pltpu.VMEM((D, 256), BF16),
                pltpu.VMEM((NGC, D, GCH), BF16),
                pltpu.VMEM((NGC, D, GCH), BF16),
                pltpu.VMEM((RING, FF, CH), BF16),
                pltpu.VMEM((2, ROWS, 128), F32),
                pltpu.VMEM((2, ROWS, 128), F32),
                pltpu.VMEM((2, ROWS, 128), F32),
                dma((NCH,)), dma((NCH,)), dma((2,)), dma((2,)), dma((2, NGC)), dma((RING,)), dma((2, 2)),
                dma((NCH,)), dma((NCH,)), dma((NCH,)), dma((NCH,)), dma((2, NCH)), dma((2, NCH)),
                dma((LAYERS, 3, 2, 2)), dma((LAYERS, 3, 2, 2)), dma((2, 2)), dma((2, 2)),
                dma((PIECES,)), dma((PIECES,)), dma((3, PIECES)), dma((3, PIECES)),
            ],
            compiler_params=pltpu.CompilerParams(
                collective_id=0, has_side_effects=True, vmem_limit_bytes=67_000_000),
            name='decoder',
        )(tokens, norm_attn, norm_mlp, jnp.asarray(turn_table()),
          wq, w_k, w_v, wo, w_gate, w_up, w_down)

    return jax.shard_map(
        body,
        mesh=mesh,
        in_specs=(row_spec, gain_spec, gain_spec, q_spec, col_spec, col_spec, o_spec, col_spec, col_spec, down_spec),
        out_specs=row_spec,
        check_vma=False,
    )
```

```python
import functools
import math

import jax
import jax.numpy as jnp
import numpy as np
from jax import lax
from jax.experimental import pallas as pl
from jax.experimental.pallas import tpu as pltpu
from jax.sharding import PartitionSpec as P

MESH = pl.DeviceIdType.MESH
F32 = jnp.float32
BF16 = jnp.bfloat16
ROWS, SEG, D, HEAD, FF = 128, 64, 2048, 64, 4096
CH, NCH = 256, 8
GCH, NGC = 512, 8
RING = 4
PIECES, PIECE = 16, 16
FIRST, MIDDLE, LATE = range(0, 4), range(4, 9), range(9, 16)
LAYERS = 2
EXP2_SCALE = math.log2(math.e) / math.sqrt(HEAD)


def kernel(tokens, gain_attn, gain_mlp, table, wq, wk, wv, wo, wg, wu, wd, out,
           x_own, x_par, a_ref, qh, o_ref, o_x, kv, act, sbuf, rbuf, slot, wo_x, wk_v, wv_v, wg_v, wu_v, wd_v,
           turns, cos_ref, sin_ref,
           tok_sem, out_sem, slot_sem, kvw_sem, gu_sem, wd_sem, wo_sem, turn_sem, xs_sem, xr_sem, ps_sem, pr_sem, ds_sem, dr_sem,
           ts_sem, tr_sem, ks_sem, kr_sem, os_sem, or_sem, ws_sem, wr_sem, fs_sem, fr_sem):
    t = lax.axis_index('tp')
    c = lax.axis_index('cp')
    other = {'tp': 1 - t}
    beside, across, corner = c + 1 - 2 * lax.rem(c, 2), lax.rem(c + 2, 4), 3 - c
    peers = (beside, across, corner)

    def load_slot(src):
        return [pltpu.make_async_copy(src.at[pl.ds(i * 512, 512)], slot.at[pl.ds(i * 512, 512)], slot_sem.at[i]) for i in range(2)]

    def load_kvw(l):
        return [pltpu.make_async_copy(wk.at[l], wk_v, kvw_sem.at[0]), pltpu.make_async_copy(wv.at[l], wv_v, kvw_sem.at[1])]

    def load_gu(l, j):
        cols = pl.ds(pl.multiple_of(j * GCH, GCH), GCH)
        return [pltpu.make_async_copy(wg.at[l, :, cols], wg_v.at[j], gu_sem.at[0, j]),
                pltpu.make_async_copy(wu.at[l, :, cols], wu_v.at[j], gu_sem.at[1, j])]

    def load_wd(l, j):
        cols = pl.ds(pl.multiple_of(j * CH, CH), CH)
        s = lax.rem(j, RING)
        return pltpu.make_async_copy(wd.at[l, :, cols], wd_v.at[s], wd_sem.at[s])

    def start(copies):
        for copy in copies:
            copy.start()

    def wait(copies):
        for copy in copies:
            copy.wait()

    def send_x(src, j):
        return pltpu.make_async_remote_copy(src, x_par.at[j], xs_sem.at[j], xr_sem.at[j], other, MESH)

    def send_tokens(i, j):
        rows, cols = pl.ds(i * SEG, SEG), pl.ds(j * CH, CH)
        return pltpu.make_async_remote_copy(tokens.at[rows, cols], x_par.at[j, rows], ts_sem.at[i, j], tr_sem.at[i, j], other, MESH)

    def load_wo(j):
        cols = pl.ds(pl.multiple_of(j * CH, CH), CH)
        return pltpu.make_async_copy(wo.at[0, :, cols], wd_v.at[lax.rem(j, RING), wo_rows(j)], wo_sem.at[j])

    def wo_rows(j):
        return pl.ds(pl.multiple_of(j // RING * 1024, 1024), 1024)

    def send_part(j):
        return pltpu.make_async_remote_copy(sbuf.at[j], rbuf.at[j], ps_sem.at[j], pr_sem.at[j], other, MESH)

    def segments(g, ti, ci):
        k = (ti if g == 0 else 1 - ti) * 4 + ci
        return k, 15 - k

    def send_half(i, j):
        place = (j, pl.ds(i * SEG, SEG))
        return pltpu.make_async_remote_copy(sbuf.at[place], rbuf.at[place], ds_sem.at[i, j], dr_sem.at[i, j], other, MESH)

    def send_o(g, i):
        rows = pl.ds(i * SEG, SEG)
        return pltpu.make_async_remote_copy(o_ref.at[g, rows], o_x.at[1 - g, rows], os_sem.at[g, i], or_sem.at[1 - g, i], other, MESH)

    def recv_o(g, i):
        rows = pl.ds(i * SEG, SEG)
        return pltpu.make_async_remote_copy(o_ref.at[g, rows], o_x.at[g, rows], os_sem.at[g, i], or_sem.at[g, i], other, MESH)

    def send_kv(l, kind, g, i, owner, to):
        rows = pl.ds(pl.multiple_of(segments(g, t, owner)[i] * SEG, SEG), SEG)
        place = kv.at[l, rows, :]
        return pltpu.make_async_remote_copy(place, place, ks_sem.at[l, kind, g, i], kr_sem.at[l, kind, g, i], {'cp': to}, MESH)

    def piece(owner, p):
        return pl.ds(pl.multiple_of(owner * (PIECES * PIECE) + p * PIECE, PIECE), PIECE)

    def send_wo(p):
        return pltpu.make_async_remote_copy(wo.at[1, piece(c, p)], wo_x.at[piece(c, p)], ws_sem.at[p], wr_sem.at[p], other, MESH)

    def spread_wo(kind, p, owner, to):
        place = wo_x.at[piece(owner, p)]
        return pltpu.make_async_remote_copy(place, place, fs_sem.at[kind, p], fr_sem.at[kind, p], {'cp': to}, MESH)

    def pass_wo(pieces):
        for p in pieces:
            send_wo(p).wait_recv()
            spread_wo(1, p, c, across).start()
            spread_wo(0, p, c, beside).start()

    def relay_wo(pieces):
        for p in pieces:
            spread_wo(1, p, across, across).wait_recv()
            spread_wo(2, p, across, beside).start()

    tok = [pltpu.make_async_copy(tokens.at[:, pl.ds(j * CH, CH)], x_own.at[j], tok_sem.at[j]) for j in range(NCH)]
    start(tok)
    turn = [pltpu.make_async_copy(table.at[pl.ds(pl.multiple_of(segments(g, t, c)[i] * SEG, SEG), SEG)],
                                  turns.at[g, pl.ds(i * SEG, SEG)], turn_sem.at[g, i]) for g in range(2) for i in range(2)]
    start(turn)
    start(load_kvw(0))
    start(load_slot(wq.at[0]))

    barrier = pltpu.get_barrier_semaphore()
    pl.semaphore_signal(barrier, inc=1, device_id=other, device_id_type=MESH)
    for to in peers:
        pl.semaphore_signal(barrier, inc=1, device_id={'cp': to}, device_id_type=MESH)
    pl.semaphore_wait(barrier, 4)
    for i in range(2):
        for j in range(NCH):
            send_tokens(i, j).start()
    for p in FIRST:
        send_wo(p).start()
    for j in range(NCH):
        load_wo(j).start()

    lane = lax.broadcasted_iota(jnp.int32, (ROWS, 128), 1)
    first_half = (lane % HEAD) < HEAD // 2
    low = lane < HEAD
    low_seg = lax.broadcasted_iota(jnp.int32, (SEG, 128), 1) < HEAD
    diff = (lax.broadcasted_iota(jnp.int32, (4 * SEG, 512), 1)
            - lax.broadcasted_iota(jnp.int32, (4 * SEG, 512), 0) % SEG)

    wait(turn)
    for g in range(2):
        near, far = turns[g], pltpu.roll(turns[g], HEAD, 1)
        cos_ref[g] = jnp.where(low, near, far)
        sin_ref[g] = jnp.where(low, far, near)

    def norm(x_ref, gain_ref, l, lo=0, n=ROWS):
        rows = pl.ds(lo, n)
        total = jnp.zeros((n, 1), F32)
        for j in range(NCH):
            x = x_ref[j, rows].astype(F32)
            total = total + jnp.sum(x * x, axis=-1, keepdims=True)
        inv = lax.rsqrt(total * (1.0 / D) + 1e-5)
        for j in range(NCH):
            cols = pl.ds(j * CH, CH)
            a_ref[rows, cols] = (x_ref[j, rows].astype(F32) * inv * gain_ref[l:l + 1, cols].astype(F32)).astype(BF16)

    def rope(v, g, rows):
        n = v.shape[0]
        swapped = jnp.where(first_half[:n], pltpu.roll(v, 128 - HEAD // 2, 1), pltpu.roll(v, HEAD // 2, 1))
        return v * cos_ref[g, rows] + swapped * sin_ref[g, rows]

    def keys_values(l, g, lo=0, n=ROWS):
        take = pl.ds(lo, n)
        k_new = jnp.dot(a_ref[take], wk_v[...], preferred_element_type=F32)
        v_new = jnp.dot(a_ref[take], wv_v[...], preferred_element_type=F32).astype(BF16)
        k_new = jnp.concatenate([rope(k_new[:, :128], g, take), rope(k_new[:, 128:], g, take)], axis=1).astype(BF16)
        parts = range(lo // SEG, (lo + n) // SEG)
        for i in parts:
            rows = pl.ds(pl.multiple_of(segments(g, t, c)[i] * SEG, SEG), SEG)
            kv[l, rows, 0:256] = k_new[i * SEG - lo:(i + 1) * SEG - lo]
            kv[l, rows, 256:512] = v_new[i * SEG - lo:(i + 1) * SEG - lo]
        for i in parts:
            for kind in ((1, 2, 0) if g == 0 else (1, 0)):
                send_kv(l, kind, g, i, c, peers[kind]).start()

    def queries(l, g, lo=0, n=ROWS):
        take = pl.ds(lo, n)
        for h in range(4):
            q = lax.dot_general(a_ref[take], slot[h * 256:(h + 1) * 256, :], (((1,), (1,)), ((), ())), preferred_element_type=F32)
            for pair in range(2):
                both = rope(q[:, pair * 128:(pair + 1) * 128], g, take)
                turned = pltpu.roll(both, HEAD, 1)
                for odd in range(2):
                    value = both if odd == h % 2 else turned
                    value = jnp.where(low[:n] if h % 2 == 0 else ~low[:n], value, 0.0).astype(BF16)
                    m = pair * 2 + odd
                    for i in range(lo // SEG, (lo + n) // SEG):
                        qh[g, i, h, m * SEG:(m + 1) * SEG, :] = value[i * SEG - lo:(i + 1) * SEG - lo]

    def attention(l, g, parts=(0, 1)):
        for i in parts:
            seg = segments(g, t, c)[i]
            free = 512 * i
            visible = diff <= seg * SEG - free

            def pair_step(p, carry, i=i, free=free, visible=visible):
                k_cols = pl.ds(pl.multiple_of(p * 128, 128), 128)
                v_cols = pl.ds(pl.multiple_of(256 + p * 128, 128), 128)
                nt = (((1,), (1,)), ((), ()))
                spans = ((free, 512), (0, 512)) if free else ((free, 512),)
                scores, tops, totals, outs = {}, {}, {}, {}
                for parity in range(2):
                    q = qh[g, i, 2 * p + parity]
                    for n, (lo, size) in enumerate(spans):
                        s = lax.dot_general(q, kv[l, pl.ds(lo, size), k_cols], nt, preferred_element_type=F32)
                        scores[parity, n] = jnp.where(visible, s, -jnp.inf) if n == 0 else s
                for parity in range(2):
                    tops[parity] = functools.reduce(jnp.maximum, [jnp.max(scores[parity, n], axis=-1, keepdims=True) for n in range(len(spans))])
                    total, mixed = 0.0, 0.0
                    for n, (lo, size) in enumerate(spans):
                        e = jnp.exp2((scores[parity, n] - tops[parity]) * EXP2_SCALE)
                        total = total + jnp.sum(e, axis=-1, keepdims=True)
                        mixed = mixed + jnp.dot(e.astype(BF16), kv[l, pl.ds(lo, size), v_cols], preferred_element_type=F32)
                    mixed = mixed / total
                    for pair in range(2):
                        sides = []
                        for odd in range(2):
                            n = pair * 2 + odd
                            value = mixed[n * SEG:(n + 1) * SEG]
                            sides.append(value if odd == parity else pltpu.roll(value, HEAD, 1))
                        cols = pl.ds(pl.multiple_of((2 * p + parity) * 256 + pair * 128, 128), 128)
                        o_ref[g, i * SEG:(i + 1) * SEG, cols] = jnp.where(low_seg, sides[0], sides[1]).astype(BF16)
                return carry
            lax.fori_loop(0, 2, pair_step, 0)

    def slot_chunk(lhs, j):
        return jnp.dot(lhs, slot[:, pl.ds(pl.multiple_of(j * CH, CH), CH)], preferred_element_type=F32)

    def reduce_chunk(own, j):
        return (x_own[j].astype(F32) + (own + rbuf[j])).astype(BF16)

    for l in range(LAYERS):
        last = l == LAYERS - 1
        if l == 0:
            wait(tok)
        norm(x_own, gain_attn, l)
        wait(load_kvw(l))
        wait(load_slot(wq.at[l]))
        keys_values(l, 0)
        queries(l, 0)

        def wait_kv(i, l=l):
            for kind, g in ((0, 0), (1, 0), (2, 0), (0, 1), (2, 1)):
                send_kv(l, kind, g, i, peers[kind], peers[kind]).wait_recv()

        def relay_kv(i, l=l):
            send_kv(l, 1, 1, i, across, across).wait_recv()
            send_kv(l, 2, 1, i, across, beside).start()

        if not last:
            for j in range(NCH):
                send_tokens(0, j).wait_recv()
            norm(x_par, gain_attn, l, 0, SEG)
            keys_values(l, 1, 0, SEG)
            queries(l, 1, 0, SEG)
            relay_kv(0)
            for j in range(NCH):
                send_tokens(1, j).wait_recv()
            norm(x_par, gain_attn, l, SEG, SEG)
            keys_values(l, 1, SEG, SEG)
            start(load_kvw(l + 1))
            for j in range(NCH):
                load_wo(j).wait()

            def wo_chunk(lhs, j):
                return jnp.dot(lhs, wd_v[lax.rem(j, RING), wo_rows(j)], preferred_element_type=F32)

            for i in range(2):
                wait_kv(i)
                attention(l, 1, (i,))

                def o_send(j, carry, i=i):
                    rows = pl.ds(i * SEG, SEG)
                    sbuf[j, rows] = wo_chunk(o_ref[1, rows], j)
                    send_half(i, j).start()
                    return carry
                lax.fori_loop(0, NCH, o_send, 0)
                if i == 0:
                    queries(l, 1, SEG, SEG)
                    start(load_slot(wq.at[l + 1]))
                    relay_kv(1)
            pass_wo(FIRST)
            attention(l, 0)

            def o_reduce(j, carry):
                own = wo_chunk(o_ref[0], j)
                start(load_gu(0, j))
                send_half(0, j).wait_recv()
                send_half(1, j).wait_recv()
                x_own[j] = reduce_chunk(own, j)
                send_x(x_own.at[j], j).start()
                return carry
            lax.fori_loop(0, NCH, o_reduce, 0)
            for p in MIDDLE:
                send_wo(p).start()
            for j in range(RING):
                load_wd(0, j).start()
            relay_wo(FIRST)
        else:
            for j in range(NCH):
                send_x(x_own.at[j], j).wait_recv()
            norm(x_par, gain_attn, l)
            keys_values(l, 1)
            queries(l, 1)
            start(load_slot(wo.at[l]))
            pass_wo(LATE[:1])
            relay_kv(0)
            pass_wo(LATE[1:3])
            relay_kv(1)
            wait_kv(0)
            pass_wo(LATE[3:4])
            attention(l, 0, (0,))
            send_o(0, 0).start()
            pass_wo(LATE[4:5])
            wait_kv(1)
            attention(l, 0, (1,))
            send_o(0, 1).start()
            pass_wo(LATE[5:6])
            attention(l, 1, (0,))
            send_o(1, 0).start()
            pass_wo(LATE[6:])
            relay_wo(LATE[:4])
            attention(l, 1, (1,))
            send_o(1, 1).start()
            wait(load_slot(wo.at[l]))

            def o_near(j, carry):
                send_part(j).wait_send()
                sbuf[j] = slot_chunk(o_ref[1], j)
                return carry
            lax.fori_loop(0, NCH, o_near, 0)
            relay_wo(LATE[4:])
            for p in range(PIECES):
                spread_wo(0, p, beside, beside).wait_recv()
                spread_wo(2, p, corner, beside).wait_recv()

        def gate_up(g, l=l, last=last):
            def step(j, carry):
                if g == (1 if last else 0):
                    wait(load_gu(l, j))
                gate = jnp.dot(a_ref[...], wg_v[j], preferred_element_type=F32)
                up = jnp.dot(a_ref[...], wu_v[j], preferred_element_type=F32)
                act[g, :, pl.ds(pl.multiple_of(j * GCH, GCH), GCH)] = (gate * jax.nn.sigmoid(gate) * up).astype(BF16)
                return carry
            lax.fori_loop(0, NGC, step, 0)

        def far_chunk(g, j):
            return jnp.dot(o_x[g], wo_x[:, pl.ds(pl.multiple_of(j * CH, CH), CH)], preferred_element_type=F32)

        if not last:
            norm(x_own, gain_mlp, l)
            gate_up(0)
            for j in range(NCH):
                send_x(x_own.at[j], j).wait_recv()
            norm(x_par, gain_mlp, l)
            gate_up(1)
        else:
            recv_o(1, 0).wait_recv()
            recv_o(1, 1).wait_recv()

            def o_far(j, carry):
                x_par[j] = (x_par[j].astype(F32) + (sbuf[j] + far_chunk(1, j))).astype(BF16)
                return carry
            lax.fori_loop(0, NCH, o_far, 0)
            norm(x_par, gain_mlp, l)
            gate_up(1)

        def down_chunk(g, j, l=l):
            load_wd(l, j).wait()
            return jnp.dot(act[g], wd_v[lax.rem(j, RING)], preferred_element_type=F32)

        def down_send(j, carry, l=l, last=last):
            part = down_chunk(1, j)
            load_wd(l, lax.rem(j + RING, NCH)).start()
            if not last:
                send_half(0, j).wait_send()
                send_half(1, j).wait_send()
            sbuf[j] = part
            send_part(j).start()
            return carry
        lax.fori_loop(0, NCH, down_send, 0)
        if not last:
            pass_wo(MIDDLE)
        else:
            recv_o(0, 0).wait_recv()
            recv_o(0, 1).wait_recv()

            def o_own(j, carry):
                new = (x_own[j].astype(F32) + (slot_chunk(o_ref[0], j) + far_chunk(0, j))).astype(BF16)
                send_x(x_own.at[j], j).wait_send()
                x_own[j] = new
                return carry
            lax.fori_loop(0, NCH, o_own, 0)
            norm(x_own, gain_mlp, l)
            gate_up(0)

        def down_reduce(j, carry, l=l, last=last):
            own = down_chunk(0, j)
            if last:
                @pl.when(j < NCH - RING)
                def _():
                    load_wd(l, j + RING).start()
            else:
                @pl.when(j < NCH - RING)
                def _():
                    load_wd(l, j + RING).start()

                @pl.when(j >= NCH - RING)
                def _():
                    load_wd(l + 1, j + RING - NCH).start()
            if not last:
                start(load_gu(l + 1, j))
            send_part(j).wait_recv()
            new = reduce_chunk(own, j)
            if not last:
                send_x(x_own.at[j], j).wait_send()
            x_own[j] = new
            cols = pl.ds(pl.multiple_of(j * CH, CH), CH)
            if last:
                pltpu.make_async_copy(x_own.at[j], out.at[:, cols], out_sem.at[j]).start()
            else:
                send_x(x_own.at[j], j).start()
            return carry
        lax.fori_loop(0, NCH, down_reduce, 0)
        if not last:
            for p in LATE:
                send_wo(p).start()
            relay_wo(MIDDLE)

    for j in range(NCH):
        send_part(j).wait_send()
        pltpu.make_async_copy(x_own.at[j], out.at[:, pl.ds(j * CH, CH)], out_sem.at[j]).wait()
    for l in range(LAYERS):
        for g in range(2):
            for i in range(2):
                for kind in range(3):
                    send_kv(l, kind, g, i, c, beside).wait_send()
    for i in range(2):
        for j in range(NCH):
            send_tokens(i, j).wait_send()
    for g in range(2):
        send_o(g, 0).wait_send()
        send_o(g, 1).wait_send()
    for p in range(PIECES):
        send_wo(p).wait_send()
        for kind in range(3):
            spread_wo(kind, p, c, beside).wait_send()


def turn_table():
    inv_freq = np.float32(500000.0) ** (-(np.arange(HEAD // 2, dtype=np.float32) * np.float32(2.0) / np.float32(HEAD)))
    angles = np.arange(16 * SEG, dtype=np.float32)[:, None] * inv_freq.astype(np.float32)[None, :]
    cos, sin = np.cos(angles), np.sin(angles)
    return np.concatenate([cos, cos, -sin, sin], axis=1).astype(np.float32)


def solution(mesh):
    tp_size = mesh.shape['tp']
    cp_size = mesh.shape['cp']
    row_spec = P(('dp', 'tp', 'cp'), None)
    gain_spec = P(None, None)
    q_spec = P(None, None, 'tp', None)
    col_spec = P(None, None, 'tp')
    o_spec = P(None, 'tp', None, None)
    down_spec = P(None, 'tp', None)

    def body(tokens, norm_attn, norm_mlp, w_q, w_k, w_v, w_o, w_gate, w_up, w_down):
        wq = jnp.transpose(w_q, (0, 2, 3, 1)).reshape(LAYERS, 1024, D)
        wo = w_o.reshape(LAYERS, 1024, D)
        hbm = pl.BlockSpec(memory_space=pl.ANY)
        vmem = pl.BlockSpec(memory_space=pltpu.VMEM)
        dma = pltpu.SemaphoreType.DMA
        return pl.pallas_call(
            kernel,
            out_shape=jax.ShapeDtypeStruct((ROWS, D), BF16),
            in_specs=[hbm, vmem, vmem] + [hbm] * 8,
            out_specs=hbm,
            scratch_shapes=[
                pltpu.VMEM((NCH, ROWS, CH), BF16),
                pltpu.VMEM((NCH, ROWS, CH), BF16),
                pltpu.VMEM((ROWS, D), BF16),
                pltpu.VMEM((2, 2, 4, 4 * SEG, 128), BF16),
                pltpu.VMEM((2, ROWS, 1024), BF16),
                pltpu.VMEM((2, ROWS, 1024), BF16),
                pltpu.VMEM((LAYERS, 1024, 512), BF16),
                pltpu.VMEM((2, ROWS, FF), BF16),
                pltpu.VMEM((NCH, ROWS, CH), F32),
                pltpu.VMEM((NCH, ROWS, CH), F32),
                pltpu.VMEM((1024, D), BF16),
                pltpu.VMEM((1024, D), BF16),
                pltpu.VMEM((D, 256), BF16),
                pltpu.VMEM((D, 256), BF16),
                pltpu.VMEM((NGC, D, GCH), BF16),
                pltpu.VMEM((NGC, D, GCH), BF16),
                pltpu.VMEM((RING, FF, CH), BF16),
                pltpu.VMEM((2, ROWS, 128), F32),
                pltpu.VMEM((2, ROWS, 128), F32),
                pltpu.VMEM((2, ROWS, 128), F32),
                dma((NCH,)), dma((NCH,)), dma((2,)), dma((2,)), dma((2, NGC)), dma((RING,)), dma((NCH,)), dma((2, 2)),
                dma((NCH,)), dma((NCH,)), dma((NCH,)), dma((NCH,)), dma((2, NCH)), dma((2, NCH)), dma((2, NCH)), dma((2, NCH)),
                dma((LAYERS, 3, 2, 2)), dma((LAYERS, 3, 2, 2)), dma((2, 2)), dma((2, 2)),
                dma((PIECES,)), dma((PIECES,)), dma((3, PIECES)), dma((3, PIECES)),
            ],
            compiler_params=pltpu.CompilerParams(
                collective_id=0, has_side_effects=True, vmem_limit_bytes=67_000_000),
            name='decoder',
        )(tokens, norm_attn, norm_mlp, jnp.asarray(turn_table()),
          wq, w_k, w_v, wo, w_gate, w_up, w_down)

    return jax.shard_map(
        body,
        mesh=mesh,
        in_specs=(row_spec, gain_spec, gain_spec, q_spec, col_spec, col_spec, o_spec, col_spec, col_spec, down_spec),
        out_specs=row_spec,
        check_vma=False,
    )
```

```python
import functools
import math

import jax
import jax.numpy as jnp
import numpy as np
from jax import lax
from jax.experimental import pallas as pl
from jax.experimental.pallas import tpu as pltpu
from jax.sharding import PartitionSpec as P

MESH = pl.DeviceIdType.MESH
F32 = jnp.float32
BF16 = jnp.bfloat16
ROWS, SEG, D, HEAD, FF = 128, 64, 2048, 64, 4096
CH, NCH, NTWO = 256, 8, 4
GCH, NGC = 512, 8
RING = 4
PIECES, PIECE = 16, 16
FIRST, MIDDLE, LATE = range(0, 4), range(4, 9), range(9, 16)
LAYERS = 2
EXP2_SCALE = math.log2(math.e) / math.sqrt(HEAD)


def kernel(tokens, gain_attn, gain_mlp, table, wq, wk, wv, wo, wg, wu, wd, out,
           x_own, x_par, a_ref, qh, o_ref, o_x, kv, act, sbuf, rbuf, slot, wo_x, wk_v, wv_v, wg_v, wu_v, wd_v,
           turns, cos_ref, sin_ref,
           tok_sem, out_sem, slot_sem, kvw_sem, gu_sem, wd_sem, wo_sem, turn_sem, xs_sem, xr_sem, ps_sem, pr_sem, ds_sem, dr_sem,
           ts_sem, tr_sem, ks_sem, kr_sem, os_sem, or_sem, ws_sem, wr_sem, fs_sem, fr_sem):
    t = lax.axis_index('tp')
    c = lax.axis_index('cp')
    other = {'tp': 1 - t}
    beside, across, corner = c + 1 - 2 * lax.rem(c, 2), lax.rem(c + 2, 4), 3 - c
    peers = (beside, across, corner)

    def load_slot(src):
        return [pltpu.make_async_copy(src.at[pl.ds(i * 512, 512)], slot.at[pl.ds(i * 512, 512)], slot_sem.at[i]) for i in range(2)]

    def load_kvw(l):
        return [pltpu.make_async_copy(wk.at[l], wk_v, kvw_sem.at[0]), pltpu.make_async_copy(wv.at[l], wv_v, kvw_sem.at[1])]

    def load_gu(l, j):
        cols = pl.ds(pl.multiple_of(j * GCH, GCH), GCH)
        return [pltpu.make_async_copy(wg.at[l, :, cols], wg_v.at[j], gu_sem.at[0, j]),
                pltpu.make_async_copy(wu.at[l, :, cols], wu_v.at[j], gu_sem.at[1, j])]

    def load_wd(l, j):
        cols = pl.ds(pl.multiple_of(j * CH, CH), CH)
        s = lax.rem(j, RING)
        return pltpu.make_async_copy(wd.at[l, :, cols], wd_v.at[s], wd_sem.at[s])

    def start(copies):
        for copy in copies:
            copy.start()

    def wait(copies):
        for copy in copies:
            copy.wait()

    def send_x(k):
        two = pl.ds(2 * k, 2)
        return pltpu.make_async_remote_copy(x_own.at[two], x_par.at[two], xs_sem.at[k], xr_sem.at[k], other, MESH)

    def send_tokens(i):
        rows = pl.ds(i * SEG, SEG)
        return pltpu.make_async_remote_copy(tokens.at[rows], act.at[1, rows, pl.ds(0, D)], ts_sem.at[i], tr_sem.at[i], other, MESH)

    def load_wo(j):
        cols = pl.ds(pl.multiple_of(j * CH, CH), CH)
        return pltpu.make_async_copy(wo.at[0, :, cols], wd_v.at[lax.rem(j, RING), wo_rows(j)], wo_sem.at[j])

    def wo_rows(j):
        return pl.ds(pl.multiple_of(j // RING * 1024, 1024), 1024)

    def send_part(k):
        two = pl.ds(2 * k, 2)
        return pltpu.make_async_remote_copy(sbuf.at[two], rbuf.at[two], ps_sem.at[k], pr_sem.at[k], other, MESH)

    def segments(g, ti, ci):
        k = (ti if g == 0 else 1 - ti) * 4 + ci
        return k, 15 - k

    def send_half(i, k):
        place = (pl.ds(2 * k, 2), pl.ds(i * SEG, SEG))
        return pltpu.make_async_remote_copy(sbuf.at[place], rbuf.at[place], ds_sem.at[i, k], dr_sem.at[i, k], other, MESH)

    def send_o(g, i):
        rows = pl.ds(i * SEG, SEG)
        return pltpu.make_async_remote_copy(o_ref.at[g, rows], o_x.at[1 - g, rows], os_sem.at[g, i], or_sem.at[1 - g, i], other, MESH)

    def recv_o(g, i):
        rows = pl.ds(i * SEG, SEG)
        return pltpu.make_async_remote_copy(o_ref.at[g, rows], o_x.at[g, rows], os_sem.at[g, i], or_sem.at[g, i], other, MESH)

    def send_kv(l, kind, g, i, owner, to):
        rows = pl.ds(pl.multiple_of(segments(g, t, owner)[i] * SEG, SEG), SEG)
        place = kv.at[l, rows, :]
        return pltpu.make_async_remote_copy(place, place, ks_sem.at[l, kind, g, i], kr_sem.at[l, kind, g, i], {'cp': to}, MESH)

    def piece(owner, p):
        return pl.ds(pl.multiple_of(owner * (PIECES * PIECE) + p * PIECE, PIECE), PIECE)

    def send_wo(p):
        return pltpu.make_async_remote_copy(wo.at[1, piece(c, p)], wo_x.at[piece(c, p)], ws_sem.at[p], wr_sem.at[p], other, MESH)

    def spread_wo(kind, p, owner, to):
        place = wo_x.at[piece(owner, p)]
        return pltpu.make_async_remote_copy(place, place, fs_sem.at[kind, p], fr_sem.at[kind, p], {'cp': to}, MESH)

    def pass_wo(pieces):
        for p in pieces:
            send_wo(p).wait_recv()
            spread_wo(1, p, c, across).start()
            spread_wo(0, p, c, beside).start()

    def relay_wo(pieces):
        for p in pieces:
            spread_wo(1, p, across, across).wait_recv()
            spread_wo(2, p, across, beside).start()

    tok = [pltpu.make_async_copy(tokens.at[:, pl.ds(j * CH, CH)], x_own.at[j], tok_sem.at[j]) for j in range(NCH)]
    start(tok)
    turn = [pltpu.make_async_copy(table.at[pl.ds(pl.multiple_of(segments(g, t, c)[i] * SEG, SEG), SEG)],
                                  turns.at[g, pl.ds(i * SEG, SEG)], turn_sem.at[g, i]) for g in range(2) for i in range(2)]
    start(turn)
    start(load_kvw(0))
    start(load_slot(wq.at[0]))

    barrier = pltpu.get_barrier_semaphore()
    pl.semaphore_signal(barrier, inc=1, device_id=other, device_id_type=MESH)
    for to in peers:
        pl.semaphore_signal(barrier, inc=1, device_id={'cp': to}, device_id_type=MESH)
    pl.semaphore_wait(barrier, 4)
    for i in range(2):
        send_tokens(i).start()
    for p in FIRST:
        send_wo(p).start()
    for j in range(NCH):
        load_wo(j).start()

    lane = lax.broadcasted_iota(jnp.int32, (ROWS, 128), 1)
    first_half = (lane % HEAD) < HEAD // 2
    low = lane < HEAD
    low_seg = lax.broadcasted_iota(jnp.int32, (SEG, 128), 1) < HEAD
    diff = (lax.broadcasted_iota(jnp.int32, (4 * SEG, 512), 1)
            - lax.broadcasted_iota(jnp.int32, (4 * SEG, 512), 0) % SEG)

    wait(turn)
    for g in range(2):
        near, far = turns[g], pltpu.roll(turns[g], HEAD, 1)
        cos_ref[g] = jnp.where(low, near, far)
        sin_ref[g] = jnp.where(low, far, near)

    def norm(x_ref, gain_ref, l, lo=0, n=ROWS):
        rows = pl.ds(lo, n)
        total = jnp.zeros((n, 1), F32)

        def chunk(j):
            return x_ref[1, rows, j * CH:(j + 1) * CH] if x_ref is act else x_ref[j, rows]

        for j in range(NCH):
            x = chunk(j).astype(F32)
            total = total + jnp.sum(x * x, axis=-1, keepdims=True)
        inv = lax.rsqrt(total * (1.0 / D) + 1e-5)
        for j in range(NCH):
            cols = pl.ds(j * CH, CH)
            a_ref[rows, cols] = (chunk(j).astype(F32) * inv * gain_ref[l:l + 1, cols].astype(F32)).astype(BF16)

    def rope(v, g, rows):
        n = v.shape[0]
        swapped = jnp.where(first_half[:n], pltpu.roll(v, 128 - HEAD // 2, 1), pltpu.roll(v, HEAD // 2, 1))
        return v * cos_ref[g, rows] + swapped * sin_ref[g, rows]

    def keys_values(l, g, lo=0, n=ROWS):
        take = pl.ds(lo, n)
        k_new = jnp.dot(a_ref[take], wk_v[...], preferred_element_type=F32)
        v_new = jnp.dot(a_ref[take], wv_v[...], preferred_element_type=F32).astype(BF16)
        k_new = jnp.concatenate([rope(k_new[:, :128], g, take), rope(k_new[:, 128:], g, take)], axis=1).astype(BF16)
        parts = range(lo // SEG, (lo + n) // SEG)
        for i in parts:
            rows = pl.ds(pl.multiple_of(segments(g, t, c)[i] * SEG, SEG), SEG)
            kv[l, rows, 0:256] = k_new[i * SEG - lo:(i + 1) * SEG - lo]
            kv[l, rows, 256:512] = v_new[i * SEG - lo:(i + 1) * SEG - lo]
        for i in parts:
            for kind in ((1, 2, 0) if g == 0 else (1, 0)):
                send_kv(l, kind, g, i, c, peers[kind]).start()

    def queries(l, g, lo=0, n=ROWS):
        take = pl.ds(lo, n)
        for h in range(4):
            q = lax.dot_general(a_ref[take], slot[h * 256:(h + 1) * 256, :], (((1,), (1,)), ((), ())), preferred_element_type=F32)
            for pair in range(2):
                both = rope(q[:, pair * 128:(pair + 1) * 128], g, take)
                turned = pltpu.roll(both, HEAD, 1)
                for odd in range(2):
                    value = both if odd == h % 2 else turned
                    value = jnp.where(low[:n] if h % 2 == 0 else ~low[:n], value, 0.0).astype(BF16)
                    m = pair * 2 + odd
                    for i in range(lo // SEG, (lo + n) // SEG):
                        qh[g, i, h, m * SEG:(m + 1) * SEG, :] = value[i * SEG - lo:(i + 1) * SEG - lo]

    def attention(l, g, parts=(0, 1)):
        for i in parts:
            seg = segments(g, t, c)[i]
            free = 512 * i
            visible = diff <= seg * SEG - free

            def pair_step(p, carry, i=i, free=free, visible=visible):
                k_cols = pl.ds(pl.multiple_of(p * 128, 128), 128)
                v_cols = pl.ds(pl.multiple_of(256 + p * 128, 128), 128)
                nt = (((1,), (1,)), ((), ()))
                spans = ((free, 512), (0, 512)) if free else ((free, 512),)
                scores, tops, totals, outs = {}, {}, {}, {}
                for parity in range(2):
                    q = qh[g, i, 2 * p + parity]
                    for n, (lo, size) in enumerate(spans):
                        s = lax.dot_general(q, kv[l, pl.ds(lo, size), k_cols], nt, preferred_element_type=F32)
                        scores[parity, n] = jnp.where(visible, s, -jnp.inf) if n == 0 else s
                for parity in range(2):
                    tops[parity] = functools.reduce(jnp.maximum, [jnp.max(scores[parity, n], axis=-1, keepdims=True) for n in range(len(spans))])
                    total, mixed = 0.0, 0.0
                    for n, (lo, size) in enumerate(spans):
                        e = jnp.exp2((scores[parity, n] - tops[parity]) * EXP2_SCALE)
                        total = total + jnp.sum(e, axis=-1, keepdims=True)
                        mixed = mixed + jnp.dot(e.astype(BF16), kv[l, pl.ds(lo, size), v_cols], preferred_element_type=F32)
                    mixed = mixed / total
                    for pair in range(2):
                        sides = []
                        for odd in range(2):
                            n = pair * 2 + odd
                            value = mixed[n * SEG:(n + 1) * SEG]
                            sides.append(value if odd == parity else pltpu.roll(value, HEAD, 1))
                        cols = pl.ds(pl.multiple_of((2 * p + parity) * 256 + pair * 128, 128), 128)
                        o_ref[g, i * SEG:(i + 1) * SEG, cols] = jnp.where(low_seg, sides[0], sides[1]).astype(BF16)
                return carry
            lax.fori_loop(0, 2, pair_step, 0)

    def slot_chunk(lhs, j):
        return jnp.dot(lhs, slot[:, pl.ds(pl.multiple_of(j * CH, CH), CH)], preferred_element_type=F32)

    def reduce_chunk(own, j):
        return (x_own[j].astype(F32) + (own + rbuf[j])).astype(BF16)

    for l in range(LAYERS):
        last = l == LAYERS - 1
        if l == 0:
            wait(tok)
        norm(x_own, gain_attn, l)
        wait(load_kvw(l))
        wait(load_slot(wq.at[l]))
        keys_values(l, 0)
        queries(l, 0)

        def wait_kv(i, l=l):
            for kind, g in ((0, 0), (1, 0), (2, 0), (0, 1), (2, 1)):
                send_kv(l, kind, g, i, peers[kind], peers[kind]).wait_recv()

        def relay_kv(i, l=l):
            send_kv(l, 1, 1, i, across, across).wait_recv()
            send_kv(l, 2, 1, i, across, beside).start()

        if not last:
            send_tokens(0).wait_recv()
            norm(act, gain_attn, l, 0, SEG)
            keys_values(l, 1, 0, SEG)
            queries(l, 1, 0, SEG)
            relay_kv(0)
            send_tokens(1).wait_recv()
            norm(act, gain_attn, l, SEG, SEG)
            keys_values(l, 1, SEG, SEG)
            start(load_kvw(l + 1))
            for j in range(NCH):
                load_wo(j).wait()

            def wo_chunk(lhs, j):
                return jnp.dot(lhs, wd_v[lax.rem(j, RING), wo_rows(j)], preferred_element_type=F32)

            for i in range(2):
                wait_kv(i)
                attention(l, 1, (i,))

                def o_send(k, carry, i=i):
                    rows = pl.ds(i * SEG, SEG)
                    for j in (2 * k, 2 * k + 1):
                        sbuf[j, rows] = wo_chunk(o_ref[1, rows], j)
                    send_half(i, k).start()
                    return carry
                lax.fori_loop(0, NTWO, o_send, 0)
                if i == 0:
                    queries(l, 1, SEG, SEG)
                    start(load_slot(wq.at[l + 1]))
                    relay_kv(1)
            pass_wo(FIRST)
            attention(l, 0)

            def o_reduce(j, carry):
                own = wo_chunk(o_ref[0], j)
                start(load_gu(0, j))

                @pl.when(lax.rem(j, 2) == 0)
                def _():
                    send_half(0, j // 2).wait_recv()
                    send_half(1, j // 2).wait_recv()
                x_own[j] = reduce_chunk(own, j)

                @pl.when(lax.rem(j, 2) == 1)
                def _():
                    send_x(j // 2).start()
                return carry
            lax.fori_loop(0, NCH, o_reduce, 0)
            for p in MIDDLE:
                send_wo(p).start()
            for j in range(RING):
                load_wd(0, j).start()
            relay_wo(FIRST)
        else:
            for k in range(NTWO):
                send_x(k).wait_recv()
            norm(x_par, gain_attn, l)
            keys_values(l, 1)
            queries(l, 1)
            start(load_slot(wo.at[l]))
            pass_wo(LATE[:1])
            relay_kv(0)
            pass_wo(LATE[1:3])
            relay_kv(1)
            wait_kv(0)
            pass_wo(LATE[3:4])
            attention(l, 0, (0,))
            send_o(0, 0).start()
            pass_wo(LATE[4:5])
            wait_kv(1)
            attention(l, 0, (1,))
            send_o(0, 1).start()
            pass_wo(LATE[5:6])
            attention(l, 1, (0,))
            send_o(1, 0).start()
            pass_wo(LATE[6:])
            relay_wo(LATE[:4])
            attention(l, 1, (1,))
            send_o(1, 1).start()
            wait(load_slot(wo.at[l]))

            for k in range(NTWO):
                send_part(k).wait_send()

            def o_near(j, carry):
                sbuf[j] = slot_chunk(o_ref[1], j)
                return carry
            lax.fori_loop(0, NCH, o_near, 0)
            relay_wo(LATE[4:])
            for p in range(PIECES):
                spread_wo(0, p, beside, beside).wait_recv()
                spread_wo(2, p, corner, beside).wait_recv()

        def gate_up(g, l=l, last=last):
            def step(j, carry):
                if g == (1 if last else 0):
                    wait(load_gu(l, j))
                gate = jnp.dot(a_ref[...], wg_v[j], preferred_element_type=F32)
                up = jnp.dot(a_ref[...], wu_v[j], preferred_element_type=F32)
                act[g, :, pl.ds(pl.multiple_of(j * GCH, GCH), GCH)] = (gate * jax.nn.sigmoid(gate) * up).astype(BF16)
                return carry
            lax.fori_loop(0, NGC, step, 0)

        def far_chunk(g, j):
            return jnp.dot(o_x[g], wo_x[:, pl.ds(pl.multiple_of(j * CH, CH), CH)], preferred_element_type=F32)

        if not last:
            norm(x_own, gain_mlp, l)
            gate_up(0)
            for k in range(NTWO):
                send_x(k).wait_recv()
            norm(x_par, gain_mlp, l)
            gate_up(1)
        else:
            recv_o(1, 0).wait_recv()
            recv_o(1, 1).wait_recv()

            def o_far(j, carry):
                x_par[j] = (x_par[j].astype(F32) + (sbuf[j] + far_chunk(1, j))).astype(BF16)
                return carry
            lax.fori_loop(0, NCH, o_far, 0)
            norm(x_par, gain_mlp, l)
            gate_up(1)

        def down_chunk(g, j, l=l):
            load_wd(l, j).wait()
            return jnp.dot(act[g], wd_v[lax.rem(j, RING)], preferred_element_type=F32)

        if not last:
            for k in range(NTWO):
                send_half(0, k).wait_send()
                send_half(1, k).wait_send()

        def down_send(j, carry, l=l):
            sbuf[j] = down_chunk(1, j)
            load_wd(l, lax.rem(j + RING, NCH)).start()

            @pl.when(lax.rem(j, 2) == 1)
            def _():
                send_part(j // 2).start()
            return carry
        lax.fori_loop(0, NCH, down_send, 0)
        if not last:
            pass_wo(MIDDLE)
        else:
            recv_o(0, 0).wait_recv()
            recv_o(0, 1).wait_recv()

            for k in range(NTWO):
                send_x(k).wait_send()

            def o_own(j, carry):
                x_own[j] = (x_own[j].astype(F32) + (slot_chunk(o_ref[0], j) + far_chunk(0, j))).astype(BF16)
                return carry
            lax.fori_loop(0, NCH, o_own, 0)
            norm(x_own, gain_mlp, l)
            gate_up(0)

        if not last:
            for k in range(NTWO):
                send_x(k).wait_send()

        def down_reduce(j, carry, l=l, last=last):
            own = down_chunk(0, j)

            @pl.when(j < NCH - RING)
            def _():
                load_wd(l, j + RING).start()
            if not last:
                @pl.when(j >= NCH - RING)
                def _():
                    load_wd(l + 1, j + RING - NCH).start()
                start(load_gu(l + 1, j))

            @pl.when(lax.rem(j, 2) == 0)
            def _():
                send_part(j // 2).wait_recv()
            x_own[j] = reduce_chunk(own, j)
            if last:
                cols = pl.ds(pl.multiple_of(j * CH, CH), CH)
                pltpu.make_async_copy(x_own.at[j], out.at[:, cols], out_sem.at[j]).start()
            else:
                @pl.when(lax.rem(j, 2) == 1)
                def _():
                    send_x(j // 2).start()
            return carry
        lax.fori_loop(0, NCH, down_reduce, 0)
        if not last:
            for p in LATE:
                send_wo(p).start()
            relay_wo(MIDDLE)

    for k in range(NTWO):
        send_part(k).wait_send()
    for j in range(NCH):
        pltpu.make_async_copy(x_own.at[j], out.at[:, pl.ds(j * CH, CH)], out_sem.at[j]).wait()
    for l in range(LAYERS):
        for g in range(2):
            for i in range(2):
                for kind in range(3):
                    send_kv(l, kind, g, i, c, beside).wait_send()
    for i in range(2):
        send_tokens(i).wait_send()
    for g in range(2):
        send_o(g, 0).wait_send()
        send_o(g, 1).wait_send()
    for p in range(PIECES):
        send_wo(p).wait_send()
        for kind in range(3):
            spread_wo(kind, p, c, beside).wait_send()


def turn_table():
    inv_freq = np.float32(500000.0) ** (-(np.arange(HEAD // 2, dtype=np.float32) * np.float32(2.0) / np.float32(HEAD)))
    angles = np.arange(16 * SEG, dtype=np.float32)[:, None] * inv_freq.astype(np.float32)[None, :]
    cos, sin = np.cos(angles), np.sin(angles)
    return np.concatenate([cos, cos, -sin, sin], axis=1).astype(np.float32)


def solution(mesh):
    tp_size = mesh.shape['tp']
    cp_size = mesh.shape['cp']
    row_spec = P(('dp', 'tp', 'cp'), None)
    gain_spec = P(None, None)
    q_spec = P(None, None, 'tp', None)
    col_spec = P(None, None, 'tp')
    o_spec = P(None, 'tp', None, None)
    down_spec = P(None, 'tp', None)

    def body(tokens, norm_attn, norm_mlp, w_q, w_k, w_v, w_o, w_gate, w_up, w_down):
        wq = jnp.transpose(w_q, (0, 2, 3, 1)).reshape(LAYERS, 1024, D)
        wo = w_o.reshape(LAYERS, 1024, D)
        hbm = pl.BlockSpec(memory_space=pl.ANY)
        vmem = pl.BlockSpec(memory_space=pltpu.VMEM)
        dma = pltpu.SemaphoreType.DMA
        return pl.pallas_call(
            kernel,
            out_shape=jax.ShapeDtypeStruct((ROWS, D), BF16),
            in_specs=[hbm, vmem, vmem] + [hbm] * 8,
            out_specs=hbm,
            scratch_shapes=[
                pltpu.VMEM((NCH, ROWS, CH), BF16),
                pltpu.VMEM((NCH, ROWS, CH), BF16),
                pltpu.VMEM((ROWS, D), BF16),
                pltpu.VMEM((2, 2, 4, 4 * SEG, 128), BF16),
                pltpu.VMEM((2, ROWS, 1024), BF16),
                pltpu.VMEM((2, ROWS, 1024), BF16),
                pltpu.VMEM((LAYERS, 1024, 512), BF16),
                pltpu.VMEM((2, ROWS, FF), BF16),
                pltpu.VMEM((NCH, ROWS, CH), F32),
                pltpu.VMEM((NCH, ROWS, CH), F32),
                pltpu.VMEM((1024, D), BF16),
                pltpu.VMEM((1024, D), BF16),
                pltpu.VMEM((D, 256), BF16),
                pltpu.VMEM((D, 256), BF16),
                pltpu.VMEM((NGC, D, GCH), BF16),
                pltpu.VMEM((NGC, D, GCH), BF16),
                pltpu.VMEM((RING, FF, CH), BF16),
                pltpu.VMEM((2, ROWS, 128), F32),
                pltpu.VMEM((2, ROWS, 128), F32),
                pltpu.VMEM((2, ROWS, 128), F32),
                dma((NCH,)), dma((NCH,)), dma((2,)), dma((2,)), dma((2, NGC)), dma((RING,)), dma((NCH,)), dma((2, 2)),
                dma((NTWO,)), dma((NTWO,)), dma((NTWO,)), dma((NTWO,)), dma((2, NTWO)), dma((2, NTWO)), dma((2,)), dma((2,)),
                dma((LAYERS, 3, 2, 2)), dma((LAYERS, 3, 2, 2)), dma((2, 2)), dma((2, 2)),
                dma((PIECES,)), dma((PIECES,)), dma((3, PIECES)), dma((3, PIECES)),
            ],
            compiler_params=pltpu.CompilerParams(
                collective_id=0, has_side_effects=True, vmem_limit_bytes=67_000_000),
            name='decoder',
        )(tokens, norm_attn, norm_mlp, jnp.asarray(turn_table()),
          wq, w_k, w_v, wo, w_gate, w_up, w_down)

    return jax.shard_map(
        body,
        mesh=mesh,
        in_specs=(row_spec, gain_spec, gain_spec, q_spec, col_spec, col_spec, o_spec, col_spec, col_spec, down_spec),
        out_specs=row_spec,
        check_vma=False,
    )
```
